32 devices in a mesh: seq: 16 (over z, y, x), batch: 2 (over core).
Axes of the slice: x: 2, y: 2, z: 4, core: 2. Of those that a mesh axis runs over, the one named last changes fastest.
Arguments:
- inputs: bfloat16 [2, 2048, 2048], P('batch', 'seq'), may hold values from -6 to 6
- cotangent: bfloat16 [2, 2048, 1024], P('batch', 'seq'), may hold values from -48 to 48
- w_query: bfloat16 [2048, 128], replicated, may hold values from -0.125 to 0.125
- w_key: bfloat16 [2048, 128], replicated, may hold values from -0.125 to 0.125
- w_value: bfloat16 [2048, 1024], replicated, may hold values from -0.125 to 0.125
Outputs:
- grad_inputs: bfloat16 [2, 2048, 2048], P('batch', 'seq')
- grad_w_query: float32 [2048, 128], P(('seq', 'batch'))
- grad_w_key: float32 [2048, 128], P(('seq', 'batch'))
- grad_w_value: float32 [2048, 1024], P(('seq', 'batch'))
The draws below stay inside these ranges and needn't reach their ends.
All inputs are finite; a program needn't handle non-finite values.
Results may differ from the reference program's by a relative error of at most 0.006.
Values sent between devices are 32-bit elements; how exact they have to be, the bound alone decides.
A program may use at most 128 MiB of HBM per device.

```python
import math
import jax
import jax.numpy as jnp
import numpy as np
from jax import lax

D = 2048
H = 8
DK = 16
DV = 128
F = 153
SEQ_LEN = 2048
SEQS = 2


def shard_levels(stream_key, shape, cuts, least, high):
    gain, own = 1.0, jax.random.fold_in(stream_key, 6)
    for position, parts in cuts:
        draws = jnp.exp(jax.random.uniform(jax.random.fold_in(own, position), (parts,), jnp.float32, least / len(cuts), high / len(cuts)))
        gain = gain * jnp.repeat(draws, shape[position] // parts).reshape([-1 if axis == position else 1 for axis in range(len(shape))])
    return gain


def bell_draw(stream_key, extent, scale, bound, cuts=(), kind=jnp.bfloat16):
    drawn = scale * jax.random.normal(stream_key, extent, jnp.float32)
    if cuts:
        drawn = drawn * shard_levels(stream_key, extent, cuts, -0.22, 0.18)
    return jnp.clip(drawn, -bound, bound).astype(kind)


def setup_inputs(seed: int = 0) -> dict:
    streams_of = jax.random.split(jax.random.key(seed), 6)
    inputs = bell_draw(streams_of[0], (SEQS, SEQ_LEN, D), 1.0, 6.0, ((0, 2), (1, 16)))
    cotangent = bell_draw(streams_of[1], (SEQS, SEQ_LEN, H * DV), 8.0, 48.0, ((0, 2), (1, 16)))
    w_query = bell_draw(streams_of[2], (D, H * DK), D ** -0.5, 0.125)
    w_key = bell_draw(streams_of[3], (D, H * DK), D ** -0.5, 0.125)
    w_value = bell_draw(streams_of[4], (D, H * DV), D ** -0.5, 0.125)
    return dict(inputs=inputs, cotangent=cotangent, w_query=w_query, w_key=w_key, w_value=w_value)


highest = lax.Precision.HIGHEST

def pair_tables(width):
    rows_idx, cols_idx = np.triu_indices(width)
    eye_table = np.eye(width, dtype=np.float32)
    left_pick = jnp.asarray(eye_table[rows_idx])
    right_pick = jnp.asarray(eye_table[cols_idx])
    pair_coef = jnp.asarray(np.where(rows_idx == cols_idx, 1.0 / math.sqrt(2.0), 1.0).astype(np.float32))
    return (left_pick, right_pick, pair_coef)

def features(scaled, tables):
    left_pick, right_pick, pair_coef = tables
    left_val = jnp.einsum('...d,pd->...p', scaled, left_pick, precision=highest)
    right_val = jnp.einsum('...d,pd->...p', scaled, right_pick, precision=highest)
    leading = jnp.ones(scaled.shape[:-1] + (1,), jnp.float32)
    return jnp.concatenate([leading, scaled, left_val * right_val * pair_coef], -1)

def pull_back(scaled, grad_feat, tables):
    left_pick, right_pick, pair_coef = tables
    width = scaled.shape[-1]
    linear_part = grad_feat[..., 1:1 + width]
    pair_grad = grad_feat[..., 1 + width:] * pair_coef
    left_val = jnp.einsum('...d,pd->...p', scaled, left_pick, precision=highest)
    right_val = jnp.einsum('...d,pd->...p', scaled, right_pick, precision=highest)
    result = linear_part + jnp.einsum('...p,pd->...d', pair_grad * right_val, left_pick, precision=highest)
    return result + jnp.einsum('...p,pd->...d', pair_grad * left_val, right_pick, precision=highest)

def reference(inputs, cotangent, w_query, w_key, w_value):
    tables = pair_tables(DK)
    flat = inputs.reshape(SEQS * SEQ_LEN, D)
    query = jnp.dot(flat, w_query, preferred_element_type=jnp.float32).reshape(SEQS, SEQ_LEN, H, DK)
    keys = jnp.dot(flat, w_key, preferred_element_type=jnp.float32).reshape(SEQS, SEQ_LEN, H, DK)
    values = jnp.dot(flat, w_value, preferred_element_type=jnp.float32).astype(jnp.bfloat16).reshape(SEQS, SEQ_LEN, H, DV)
    feat_q = features(query * 0.5, tables).astype(jnp.bfloat16)
    feat_k = features(keys * 0.5, tables).astype(jnp.bfloat16)
    upstream = cotangent.astype(jnp.float32).reshape(SEQS, SEQ_LEN, H, DV)
    block_len = math.gcd(512, SEQ_LEN)
    nblocks = SEQ_LEN // block_len

    def blocked(array):
        return array.reshape((SEQS, nblocks, block_len) + array.shape[2:]).swapaxes(0, 1)

    def unblocked(array):
        return array.swapaxes(0, 1).reshape((SEQS, SEQ_LEN) + array.shape[3:])
    causal = lax.broadcasted_iota(jnp.int32, (block_len, block_len), 0) >= lax.broadcasted_iota(jnp.int32, (block_len, block_len), 1)

    def scores(fq32, fk32):
        attn = jnp.einsum('bthf,bshf->bhts', fq32, fk32, precision=highest)
        return jnp.where(causal, attn, 0.0)

    def grad_scores(grad_numer, grad_denom, val32):
        inner = jnp.einsum('bthe,bshe->bhts', grad_numer, val32, precision=highest)
        inner = inner + jnp.transpose(grad_denom, (0, 2, 1))[:, :, :, None]
        return jnp.where(causal, inner, 0.0)

    def forward_step(carry, pieces):
        state, norm_state = carry
        fq_blk, fk_blk, val_blk, up_blk = pieces
        fq32 = fq_blk.astype(jnp.float32)
        fk32 = fk_blk.astype(jnp.float32)
        val32 = val_blk.astype(jnp.float32)
        attn = scores(fq32, fk32)
        numerator = jnp.einsum('bhts,bshe->bthe', attn, val32, precision=highest)
        numerator = numerator + jnp.einsum('bthf,bhfe->bthe', fq32, state, precision=highest)
        denominator = jnp.transpose(lax.optimization_barrier(jnp.sum(attn, -1)), (0, 2, 1))
        denominator = denominator + jnp.einsum('bthf,bhf->bth', fq32, norm_state, precision=highest)
        output = numerator / denominator[..., None]
        grad_numer = up_blk / denominator[..., None]
        grad_denom = -lax.optimization_barrier(jnp.sum(up_blk * output, -1)) / denominator
        grad_attn = grad_scores(grad_numer, grad_denom, val32)
        grad_fq = jnp.einsum('bhts,bshf->bthf', grad_attn, fk32, precision=highest)
        grad_fq = grad_fq + jnp.einsum('bhfe,bthe->bthf', state, grad_numer, precision=highest)
        grad_fq = grad_fq + norm_state[:, None, :, :] * grad_denom[..., None]
        state = state + jnp.einsum('bshf,bshe->bhfe', fk32, val32, precision=highest)
        norm_state = norm_state + lax.optimization_barrier(jnp.sum(fk32, 1))
        return ((state, norm_state), (grad_numer, grad_denom, grad_fq))
    start_state = (jnp.zeros((SEQS, H, F, DV), jnp.float32), jnp.zeros((SEQS, H, F), jnp.float32))
    _, (grad_numer, grad_denom, grad_fq) = lax.scan(forward_step, start_state, (blocked(feat_q), blocked(feat_k), blocked(values), blocked(upstream)))

    def reverse_step(carry, pieces):
        back_state, back_norm = carry
        fq_blk, fk_blk, val_blk, numer_blk, denom_blk = pieces
        fq32 = fq_blk.astype(jnp.float32)
        fk32 = fk_blk.astype(jnp.float32)
        val32 = val_blk.astype(jnp.float32)
        attn = scores(fq32, fk32)
        grad_attn = grad_scores(numer_blk, denom_blk, val32)
        grad_val = jnp.einsum('bhts,bthe->bshe', attn, numer_blk, precision=highest)
        grad_val = grad_val + jnp.einsum('bshf,bhfe->bshe', fk32, back_state, precision=highest)
        grad_fk = jnp.einsum('bhts,bthf->bshf', grad_attn, fq32, precision=highest)
        grad_fk = grad_fk + jnp.einsum('bshe,bhfe->bshf', val32, back_state, precision=highest)
        grad_fk = grad_fk + back_norm[:, None, :, :]
        back_state = back_state + jnp.einsum('bthf,bthe->bhfe', fq32, numer_blk, precision=highest)
        back_norm = back_norm + jnp.einsum('bthf,bth->bhf', fq32, denom_blk, precision=highest)
        return ((back_state, back_norm), (grad_val, grad_fk))
    _, (grad_val, grad_fk) = lax.scan(reverse_step, start_state, (blocked(feat_q), blocked(feat_k), blocked(values), grad_numer, grad_denom), reverse=True)
    grad_fq = unblocked(grad_fq)
    grad_fk = unblocked(grad_fk)
    grad_val = unblocked(grad_val)
    grad_query = (pull_back(query * 0.5, grad_fq, tables) * 0.5).astype(jnp.bfloat16).reshape(SEQS * SEQ_LEN, H * DK)
    grad_keys = (pull_back(keys * 0.5, grad_fk, tables) * 0.5).astype(jnp.bfloat16).reshape(SEQS * SEQ_LEN, H * DK)
    grad_values = grad_val.astype(jnp.bfloat16).reshape(SEQS * SEQ_LEN, H * DV)
    grad_in = jnp.dot(grad_query, w_query.T, preferred_element_type=jnp.float32)
    grad_in = grad_in + jnp.dot(grad_keys, w_key.T, preferred_element_type=jnp.float32)
    grad_in = grad_in + jnp.dot(grad_values, w_value.T, preferred_element_type=jnp.float32)
    grad_in = grad_in.astype(jnp.bfloat16).reshape(SEQS, SEQ_LEN, D)
    grad_wq = jnp.dot(flat.T, grad_query, preferred_element_type=jnp.float32)
    grad_wk = jnp.dot(flat.T, grad_keys, preferred_element_type=jnp.float32)
    grad_wv = jnp.dot(flat.T, grad_values, preferred_element_type=jnp.float32)
    return (grad_in, grad_wq, grad_wk, grad_wv)
```

```python
import functools
import math

import jax
import jax.numpy as jnp
from jax import lax
from jax.experimental import pallas as pl
from jax.experimental.pallas import tpu as pltpu
from jax.sharding import PartitionSpec as P

H = 8
DK = 16
DV = 128
AUX = 16
PAIRS = DK * (DK + 1) // 2
FEATS = PAIRS + DK + 8
HALF = DK + DV // 2
PIECES = 2
ROWS = HALF // PIECES
BITS = (1, 2, 4)
MESH = pl.DeviceIdType.MESH
BF = jnp.bfloat16
F32 = jnp.float32
VMEM = pl.BlockSpec(memory_space=pltpu.VMEM)
HBM = pl.BlockSpec(memory_space=pl.ANY)


def push(src, dst, send, recv, device):
    copy = pltpu.make_async_remote_copy(
        src_ref=src,
        dst_ref=dst,
        send_sem=send,
        recv_sem=recv,
        device_id=device,
        device_id_type=MESH,
    )
    copy.start()
    return copy


def sems(*sizes):
    return pltpu.SemaphoreType.DMA(sizes)


def dot(left, right, dims):
    return lax.dot_general(left, right, ((dims[:1], dims[1:]), ((), ())), preferred_element_type=F32)


def halves(a):
    high = a.astype(BF)
    return high, (a - high.astype(F32)).astype(BF)


def dot2(pair, right, dims):
    return dot(pair[0], right, dims) + dot(pair[1], right, dims)


def dot2r(left, pair, dims):
    return dot(left, pair[0], dims) + dot(left, pair[1], dims)


def dot3(lefts, rights, dims):
    return (
        dot(lefts[0], rights[0], dims)
        + dot(lefts[0], rights[1], dims)
        + dot(lefts[1], rights[0], dims)
    )


def flip(rank, mask):
    for bit in BITS:
        if mask & bit:
            rank = rank + bit - 2 * bit * ((rank // bit) % 2)
    return rank


def phi(u):
    half = DK // 2
    lanes = u.shape[1]
    pieces = [u * u * math.sqrt(0.5)]
    for s in range(1, half):
        pieces.append(u * pltpu.roll(u, DK - s, 0))
    pieces.append(u[:half] * u[half:])
    pieces.append(u)
    pieces.append((lax.broadcasted_iota(jnp.int32, (8, lanes), 0) == 0).astype(F32))
    return jnp.concatenate(pieces, 0)


def pull(u, grad):
    half = DK // 2
    total = grad[PAIRS : PAIRS + DK] + grad[:DK] * u * math.sqrt(2.0)
    for s in range(1, half):
        piece = grad[s * DK : (s + 1) * DK]
        total = total + piece * pltpu.roll(u, DK - s, 0) + pltpu.roll(piece * u, s, 0)
    last = grad[half * DK : half * DK + half]
    return total + jnp.concatenate([last * u[half:], last * u[:half]], 0)


def pack(values, norms):
    low = norms[:8, :DV]
    high = jnp.concatenate([norms[:8, DV:], jnp.zeros((8, 2 * DV - FEATS), F32)], 1)
    return jnp.concatenate([values, low, high], 0)


def unpack(packed):
    values = packed[:FEATS]
    norms = jnp.concatenate([packed[FEATS : FEATS + 8], packed[FEATS + 8 :, : FEATS - DV]], 1)
    return values, jnp.concatenate([norms, jnp.zeros((AUX - 8, FEATS), F32)], 0)


def fused_kernel(
    ng, x_hbm, c_hbm, wq_hbm, wk_hbm, wv_hbm, gi_ref, out_ref,
    x_ref, c_ref, wq_ref, wk_ref, wv_ref, own, rec, st, xg, xp, xb,
    fqs, fks, vas, ah, al, nh, nl, tops, pv, rv, gvs, gfks,
    ssend, srecv, rsend, rrecv, o, gj, ls, lr, ret, jt, f2, fs,
    load, us, ur, qs, qr, xs, xr, ps, pr, ss, sr, rs, rr, gs, gr, ts, tr, bs, br, ds, dr,
):
    seq = lax.axis_index("seq")
    core = lax.axis_index("batch")
    other = 1 - core
    g = seq // H
    r = seq % H
    anti = H - 1 - r
    length = x_ref.shape[0]
    width = x_ref.shape[1]
    owned = width // (ng * H)
    slots = 2 * ng
    chunks = H // 2
    span = 2 * length

    def mate(k):
        return (g * H + flip(r, k), core)

    loads = []
    for n, (src, dst) in enumerate(
        ((c_hbm, c_ref), (x_hbm, x_ref), (wq_hbm, wq_ref), (wk_hbm, wk_ref), (wv_hbm, wv_ref))
    ):
        copy = pltpu.make_async_copy(src, dst, load.at[n])
        copy.start()
        loads.append(copy)

    peers = [mate(k) for k in range(1, H)] + [(seq, other)]
    peers += [(g * H + flip(r, bit), other) for bit in BITS]
    for d in range(1, ng):
        far = (g + d) % ng
        peers += [(far * H + r, core), (far * H + anti, core)]
    barrier = pltpu.get_barrier_semaphore()
    for peer in peers:
        pl.semaphore_signal(barrier, inc=1, device_id=peer, device_id_type=MESH)

    everything = []
    cut = 2 * DK + DV
    loads[0].wait()
    for h in range(H):
        own[h, cut:, :] = c_ref[:, h * DV : (h + 1) * DV].astype(F32).T
    pl.semaphore_wait(barrier, len(peers))
    ups = []
    for k in range(1, H):
        src = own.at[flip(r, k), pl.ds(cut, DV)]
        ups.append(push(src, rec.at[r, pl.ds(cut, DV)], us.at[k], ur.at[k], mate(k)))
    loads[1].wait()
    x = x_ref[...]
    for n, w_ref in enumerate((wq_ref, wk_ref)):
        loads[2 + n].wait()
        flat = dot(x, w_ref[...], (1, 0)).T
        for h in range(H):
            own[h, n * DK : (n + 1) * DK, :] = flat[h * DK : (h + 1) * DK]
    loads[4].wait()
    for h in range(H):
        own[h, 2 * DK : cut, :] = dot(x, wv_ref[:, h * DV : (h + 1) * DV], (1, 0)).T
    qkv = []
    for k in range(1, H):
        src = own.at[flip(r, k), pl.ds(0, cut)]
        qkv.append(push(src, rec.at[r, pl.ds(0, cut)], qs.at[k], qr.at[k], mate(k)))
    rec[r] = own[r]

    for cls in range(H // 2):
        for a in range(slots):
            at = ((a // 2) * H + (cls if a % 2 == 0 else H - 1 - cls)) * owned
            st[cls, :, a * owned : (a + 1) * owned] = x_ref[:, at : at + owned].astype(F32)

    def kind(rank):
        return rank + (rank // 4) * (H - 1 - 2 * rank)

    def exchange(ks):
        return [
            push(st.at[kind(flip(r, k))], xg.at[r], xs.at[k], xr.at[k], mate(k)) for k in ks
        ]

    shares = exchange((1, 2, 3))
    xg[r] = st[kind(r)]

    causal = lax.broadcasted_iota(jnp.int32, (span, span), 0) <= lax.broadcasted_iota(
        jnp.int32, (span, span), 1
    )
    ones = (lax.broadcasted_iota(jnp.int32, (AUX, span), 0) == 0).astype(F32)
    first = lax.broadcasted_iota(jnp.int32, (AUX, span), 0) == 0

    def part(c, start, count):
        rows = slice(start, start + count)
        return jnp.concatenate([rec[2 * c, rows, :], rec[2 * c + 1, rows, :]], 1)

    for copy in ups + qkv:
        copy.wait_recv()

    values = jnp.zeros((FEATS, DV), F32)
    norms = jnp.zeros((AUX, FEATS), F32)
    norm_at = []
    for c in range(chunks):
        fq = phi(part(c, 0, DK) * 0.5).astype(BF)
        fk = phi(part(c, DK, DK) * 0.5).astype(BF)
        va = jnp.concatenate([part(c, 2 * DK, DV), ones], 0).astype(BF)
        fqs[c] = fq
        fks[c] = fk
        vas[c] = va
        pv[c] = values
        norm_at.append(norms)
        values = values + dot(fk, va[:DV], (1, 1))
        norms = norms + dot(va[DV:], fk, (1, 1))
    ssend[...] = pack(values, norms)
    states = []
    for d in range(1, ng):
        to = (((g + d) % ng) * H + r, core)
        states.append(push(ssend, srecv.at[d], ss.at[d], sr.at[d], to))
    shares += exchange((4, 5))

    for c in range(chunks):
        fq, fk, va = fqs[c], fks[c], vas[c]
        attn = halves(jnp.where(causal, dot(fk, fq, (0, 0)), 0.0))
        ah[c] = attn[0]
        al[c] = attn[1]
        top = dot2r(va, attn, (1, 0))
        if c > 0:
            top = top + jnp.concatenate(
                [dot2(halves(pv[c]), fq, (0, 0)), dot2(halves(norm_at[c]), fq, (1, 0))], 0
            )
        tops[c] = top

    packed = jnp.zeros(ssend.shape, F32)
    for d, copy in enumerate(states, 1):
        copy.wait_recv()
        packed = packed + jnp.where((g - d + ng) % ng < g, srecv[d], 0.0)
    in_values, in_norms = unpack(packed)
    in_pair, in_norm_pair = halves(in_values), halves(in_norms)

    back = jnp.zeros((FEATS, DV), F32)
    back_norm = jnp.zeros((AUX, FEATS), F32)
    back_norm_at = [None] * chunks
    for c in reversed(range(chunks)):
        fq = fqs[c]
        top = tops[c] + jnp.concatenate(
            [dot2(in_pair, fq, (0, 0)), dot2(in_norm_pair, fq, (1, 0))], 0
        )
        scale = 1.0 / top[DV : DV + 1]
        numer = part(c, cut, DV) * scale
        denom = -jnp.sum(numer * top[:DV], 0, keepdims=True) * scale
        gn = halves(jnp.concatenate([numer, jnp.where(first, denom, 0.0)], 0))
        nh[c] = gn[0]
        nl[c] = gn[1]
        rv[c] = back
        back_norm_at[c] = back_norm
        back = back + dot2r(fq, (gn[0][:DV], gn[1][:DV]), (1, 1))
        back_norm = back_norm + dot2((gn[0][DV:], gn[1][DV:]), fq, (1, 1))
    rsend[...] = pack(back, back_norm)
    backs = []
    for d in range(1, ng):
        to = (((g + d) % ng) * H + r, core)
        backs.append(push(rsend, rrecv.at[d], rs.at[d], rr.at[d], to))
    shares += exchange((6, 7))

    def store(c, start, rows):
        half = 0 if start < HALF else 1
        at = start - half * HALF
        for b in range(2):
            o[2 * c + b, half, at : at + rows.shape[0], :] = rows[:, b * length : (b + 1) * length]

    for c in range(chunks):
        fq, fk, va = fqs[c], fks[c], vas[c]
        attn = (ah[c], al[c])
        gn = (nh[c], nl[c])
        ga = halves(jnp.where(causal, dot2r(va, gn, (0, 0)), 0.0))
        held = halves(pv[c] + in_values)
        held_norm = halves(norm_at[c] + in_norms)
        gfq = dot2r(fk, ga, (1, 0))
        gfq = gfq + dot3(held, (gn[0][:DV], gn[1][:DV]), (1, 0))
        gfq = gfq + dot3(held_norm, (gn[0][DV:], gn[1][DV:]), (0, 0))
        store(c, 0, pull(part(c, 0, DK) * 0.5, gfq) * 0.5)
        gv = dot3((gn[0][:DV], gn[1][:DV]), attn, (1, 1))
        gfk = dot2r(fq, ga, (1, 1))
        if c < chunks - 1:
            after = halves(rv[c])
            gv = gv + dot2(after, fk, (0, 0))
            gfk = gfk + dot2(after, va[:DV], (1, 0))
            gfk = gfk + dot2(halves(back_norm_at[c]), va[DV:], (0, 0))
        gvs[c] = gv
        gfks[c] = gfk

    base = (r // 4) * 4
    for copy in shares[:3]:
        copy.wait_recv()
    pairs = [push(xg.at[pl.ds(base, 4)], xp.at[pl.ds(base, 4)], ps.at[0], pr.at[0], (seq, other))]

    packed = jnp.zeros(rsend.shape, F32)
    for d, copy in enumerate(backs, 1):
        copy.wait_recv()
        packed = packed + jnp.where((g - d + ng) % ng > g, rrecv[d], 0.0)
    in_values, in_norms = unpack(packed)
    in_pair, in_norm_pair = halves(in_values), halves(in_norms)
    for c in range(chunks):
        fk, va = fks[c], vas[c]
        gv = gvs[c] + dot2(in_pair, fk, (0, 0))
        gfk = gfks[c] + dot2(in_pair, va[:DV], (1, 0)) + dot2(in_norm_pair, va[DV:], (0, 0))
        store(c, DK, gv[: DV // 2])
        store(c, HALF + DK, gv[DV // 2 :])
        store(c, HALF, pull(part(c, DK, DK) * 0.5, gfk) * 0.5)

    gathers = []
    for i in range(PIECES):
        row = []
        for n, bit in enumerate(BITS, 1):
            for half in range(2):
                row.append(
                    push(
                        o.at[:, half, pl.ds(i * ROWS, ROWS)],
                        gj.at[i, n, core],
                        gs.at[i, n, half],
                        gr.at[i, n, core],
                        (g * H + flip(r, bit), half),
                    )
                )
        row.append(
            push(
                o.at[:, other, pl.ds(i * ROWS, ROWS)],
                gj.at[i, 0, core],
                gs.at[i, 0, 0],
                gr.at[i, 0, core],
                (seq, other),
            )
        )
        gathers.append(row)
    returns = []
    for k in range(1, H):
        returns.append(push(o.at[flip(r, k)], ret.at[r], ts.at[k], tr.at[k], mate(k)))
    ret[r] = o[r]
    for i in range(PIECES):
        gj[i, 0, core] = o[:, core, i * ROWS : (i + 1) * ROWS, :]

    for copy in shares[3:]:
        copy.wait_recv()
    far = 4 - base
    pairs.append(push(xg.at[pl.ds(far, 4)], xp.at[pl.ds(far, 4)], ps.at[1], pr.at[1], (seq, other)))
    for j in range(H):
        xb[core, j * length : (j + 1) * length, :] = xg[j].astype(BF)
    for copy in pairs:
        copy.wait_recv()
    for j in range(H):
        xb[other, j * length : (j + 1) * length, :] = xp[j].astype(BF)

    def arrive(i, n, b):
        return pltpu.make_async_copy(gj.at[i, n, b], gj.at[i, n, b], gr.at[i, n, b])

    tokens = 2 * H * length
    sent = []
    for i in range(PIECES):
        for n in range(1, 1 + len(BITS)):
            for b in range(2):
                arrive(i, n, b).wait()
        arrive(i, 0, other).wait()
        rows = []
        for n in range(1 + len(BITS)):
            rows.append(
                jnp.concatenate([gj[i, n, b, j] for b in range(2) for j in range(H)], 1)
            )
        grads = jnp.concatenate(rows, 0).astype(BF)
        product = dot(grads, xb[...].reshape(tokens, slots * owned), (1, 0))
        for a in range(slots):
            ls[i, a] = product[:, a * owned : (a + 1) * owned]
        row = []
        for d in range(ng):
            for w in range(2):
                if d == 0 and w == 0:
                    continue
                group = (g + d) % ng
                rank = r if w == 0 else anti
                slot = group * 2 + rank // 4
                row.append(
                    push(
                        ls.at[i, slot], lr.at[i, d, w], bs.at[i, d, w], br.at[i, d, w],
                        (group * H + rank, core),
                    )
                )
        sent.append(row)

    for copy in returns:
        copy.wait_recv()
    blocks = []
    for n in range(2):
        blocks.append(jnp.concatenate([ret[h, n, :DK, :] for h in range(H)], 0))
    for h in range(H):
        blocks.append(jnp.concatenate([ret[h, 0, DK:, :], ret[h, 1, DK:, :]], 0))
    for n, block in enumerate(blocks):
        jt[:, n * DV : (n + 1) * DV] = block.T.astype(BF)
    step = 512
    for at in range(0, width, step):
        rows = slice(at, at + step)
        total = dot(jt[:, :DV], wq_ref[rows, :], (1, 1))
        total = total + dot(jt[:, DV : 2 * DV], wk_ref[rows, :], (1, 1))
        total = total + dot(jt[:, 2 * DV :], wv_ref[rows, :], (1, 1))
        gi_ref[:, rows] = total.astype(BF)

    swaps = []
    for i in range(PIECES):
        for copy in sent[i]:
            copy.wait_recv()
        mine = ls[i, g * 2 + r // 4]
        rest = lr[i, 0, 1]
        for d in range(1, ng):
            mine = mine + lr[i, d, 0]
            rest = rest + lr[i, d, 1]
        for n, bit in enumerate((0,) + BITS):
            f2[core, i, flip(r, bit)] = mine[n * ROWS : (n + 1) * ROWS]
            f2[core, i, flip(anti, bit)] = rest[n * ROWS : (n + 1) * ROWS]
        swaps.append(
            push(f2.at[core, i], f2.at[core, i], ds.at[i], dr.at[i], (seq, other))
        )
    for copy in swaps:
        copy.wait_recv()
    final = []
    for n in range(2):
        final.append(jnp.concatenate([f2[n, 0, h, :DK] for h in range(H)], 0))
    for h in range(H):
        parts = []
        for n in range(2):
            for i in range(PIECES):
                parts.append(f2[n, i, h, DK if i == 0 else 0 :])
        final.append(jnp.concatenate(parts, 0))
    keep = owned // 2
    for n, block in enumerate(final):
        fs[n] = block.T
        out_ref[n] = fs[n, pl.ds(pl.multiple_of(core * keep, keep), keep), :]
    everything += ups + qkv + shares + states + backs + pairs + returns + swaps
    for row in gathers + sent:
        everything += row
    for copy in everything:
        copy.wait_send()


def fused(tokens, upstream, weights, ng):
    length, width = tokens.shape
    owned = width // (ng * H)
    slots = 2 * ng
    chunks, span = H // 2, 2 * length
    vm = lambda *shape: pltpu.VMEM(shape, F32)
    half = lambda *shape: pltpu.VMEM(shape, BF)
    nb = 1 + len(BITS)
    scratch = [half(length, width), half(length, H * DV)]
    scratch += [pltpu.VMEM(w.shape, w.dtype) for w in weights]
    scratch += [
        vm(H, 2 * DK + 2 * DV, length), vm(H, 2 * DK + 2 * DV, length),
        vm(H // 2, length, slots * owned), vm(H, length, slots * owned),
        vm(H, length, slots * owned), half(2, H * length, slots * owned),
        half(chunks, FEATS, span), half(chunks, FEATS, span), half(chunks, DV + AUX, span),
        half(chunks, span, span), half(chunks, span, span),
        half(chunks, DV + AUX, span), half(chunks, DV + AUX, span),
        vm(chunks, DV + AUX, span), vm(chunks, FEATS, DV), vm(chunks, FEATS, DV),
        vm(chunks, DV, span), vm(chunks, FEATS, span),
        vm(FEATS + 16, DV), vm(ng, FEATS + 16, DV), vm(FEATS + 16, DV), vm(ng, FEATS + 16, DV),
        vm(H, 2, HALF, length), vm(PIECES, nb, 2, H, ROWS, length),
        vm(PIECES, slots, nb * ROWS, owned), vm(PIECES, ng, 2, nb * ROWS, owned),
        vm(H, 2, HALF, length), half(length, H * DV + 2 * DV),
        vm(2, PIECES, H, ROWS, owned), vm(2 + H, owned, DV),
        sems(5),
        sems(H), sems(H), sems(H), sems(H), sems(H), sems(H), sems(2), sems(2),
        sems(ng), sems(ng), sems(ng), sems(ng),
        sems(PIECES, nb, 2), sems(PIECES, nb, 2), sems(H), sems(H),
        sems(PIECES, ng, 2), sems(PIECES, ng, 2), sems(PIECES), sems(PIECES),
    ]
    return pl.pallas_call(
        functools.partial(fused_kernel, ng),
        out_shape=[
            jax.ShapeDtypeStruct((length, width), BF),
            jax.ShapeDtypeStruct((2 + H, owned // 2, DV), F32),
        ],
        in_specs=[HBM] * 5,
        out_specs=[VMEM] * 2,
        scratch_shapes=scratch,
        compiler_params=pltpu.CompilerParams(
            collective_id=0, has_side_effects=True, vmem_limit_bytes=60 << 20
        ),
    )(tokens, upstream, *weights)


def finish_kernel(gi_ref, o_ref, in_ref, oq_ref, ok_ref, ov_ref):
    in_ref[0] = gi_ref[...]
    oq_ref[...] = o_ref[0]
    ok_ref[...] = o_ref[1]
    for n in range(H):
        ov_ref[:, n * DV : (n + 1) * DV] = o_ref[2 + n]


def finish(grad_in, blocks):
    _, rows, lanes = blocks.shape
    return pl.pallas_call(
        finish_kernel,
        out_shape=[
            jax.ShapeDtypeStruct((1,) + grad_in.shape, BF),
            jax.ShapeDtypeStruct((rows, lanes), F32),
            jax.ShapeDtypeStruct((rows, lanes), F32),
            jax.ShapeDtypeStruct((rows, H * lanes), F32),
        ],
        in_specs=[VMEM] * 2,
        out_specs=[VMEM] * 4,
    )(grad_in, blocks)


def body(inputs, cotangent, w_query, w_key, w_value):
    ng = lax.axis_size("seq") // H
    weights = (w_query, w_key, w_value)
    return tuple(finish(*fused(inputs[0], cotangent[0], weights, ng)))


def solution(mesh):
    in_specs = (P("batch", "seq", None), P("batch", "seq", None), P(), P(), P())
    out_specs = (
        P("batch", "seq", None),
        P(("seq", "batch"), None),
        P(("seq", "batch"), None),
        P(("seq", "batch"), None),
    )
    return jax.shard_map(body, mesh=mesh, in_specs=in_specs, out_specs=out_specs, check_vma=False)
```

```python
import functools
import math

import jax
import jax.numpy as jnp
from jax import lax
from jax.experimental import pallas as pl
from jax.experimental.pallas import tpu as pltpu
from jax.sharding import PartitionSpec as P

H = 8
DK = 16
DV = 128
AUX = 16
PAIRS = DK * (DK + 1) // 2
FEATS = PAIRS + DK + 8
HALF = DK + DV // 2
PIECES = 5
ROWS = HALF // PIECES
BITS = (1, 2, 4)
PLANE = 4
MESH = pl.DeviceIdType.MESH
BF = jnp.bfloat16
F32 = jnp.float32
VMEM = pl.BlockSpec(memory_space=pltpu.VMEM)
HBM = pl.BlockSpec(memory_space=pl.ANY)


def push(src, dst, send, recv, device):
    copy = pltpu.make_async_remote_copy(
        src_ref=src,
        dst_ref=dst,
        send_sem=send,
        recv_sem=recv,
        device_id=device,
        device_id_type=MESH,
    )
    copy.start()
    return copy


def sems(*sizes):
    return pltpu.SemaphoreType.DMA(sizes)


def dot(left, right, dims):
    return lax.dot_general(left, right, ((dims[:1], dims[1:]), ((), ())), preferred_element_type=F32)


def halves(a):
    high = a.astype(BF)
    return high, (a - high.astype(F32)).astype(BF)


def dot2(pair, right, dims):
    return dot(pair[0], right, dims) + dot(pair[1], right, dims)


def dot2r(left, pair, dims):
    return dot(left, pair[0], dims) + dot(left, pair[1], dims)


def dot3(lefts, rights, dims):
    return (
        dot(lefts[0], rights[0], dims)
        + dot(lefts[0], rights[1], dims)
        + dot(lefts[1], rights[0], dims)
    )


def flip(rank, mask):
    for bit in BITS:
        if mask & bit:
            rank = rank + bit - 2 * bit * ((rank // bit) % 2)
    return rank


def phi(u):
    half = DK // 2
    lanes = u.shape[1]
    pieces = [u * u * math.sqrt(0.5)]
    for s in range(1, half):
        pieces.append(u * pltpu.roll(u, DK - s, 0))
    pieces.append(u[:half] * u[half:])
    pieces.append(u)
    pieces.append((lax.broadcasted_iota(jnp.int32, (8, lanes), 0) == 0).astype(F32))
    return jnp.concatenate(pieces, 0)


def pull(u, grad):
    half = DK // 2
    total = grad[PAIRS : PAIRS + DK] + grad[:DK] * u * math.sqrt(2.0)
    for s in range(1, half):
        piece = grad[s * DK : (s + 1) * DK]
        total = total + piece * pltpu.roll(u, DK - s, 0) + pltpu.roll(piece * u, s, 0)
    last = grad[half * DK : half * DK + half]
    return total + jnp.concatenate([last * u[half:], last * u[:half]], 0)


def pack(values, norms):
    low = norms[:8, :DV]
    high = jnp.concatenate([norms[:8, DV:], jnp.zeros((8, 2 * DV - FEATS), F32)], 1)
    return jnp.concatenate([values, low, high], 0)


def unpack(packed):
    values = packed[:FEATS]
    norms = jnp.concatenate([packed[FEATS : FEATS + 8], packed[FEATS + 8 :, : FEATS - DV]], 1)
    return values, jnp.concatenate([norms, jnp.zeros((AUX - 8, FEATS), F32)], 0)


def fused_kernel(
    ng, x_hbm, c_hbm, wq_hbm, wk_hbm, wv_hbm, gi_ref, out_ref,
    x_ref, c_ref, wq_ref, wk_ref, wv_ref, own, rec, st, xg, xp, xb,
    fqs, fks, vas, ah, al, nh, nl, tops, pv, rv, gvs, gfks,
    ssend, srecv, sin, rsend, rrecv, rin, o, gj, ls, lr, rt, jt, f2, fs,
    load, us, ur, qs, qr, xs, xr, zs, zr, ps, pr, ss, sr, rs, rr,
    gs, gr, hs, ts, tr, bs, br, ds, dr,
):
    seq = lax.axis_index("seq")
    core = lax.axis_index("batch")
    other = 1 - core
    g = seq // H
    r = seq % H
    mirror = flip(r, PLANE)
    length = x_ref.shape[0]
    width = x_ref.shape[1]
    owned = width // (ng * H)
    slots = 2 * ng
    chunks = H // 2
    span = 2 * length

    def mate(k):
        return (g * H + flip(r, k), core)

    loads = []
    for n, (src, dst) in enumerate(
        ((c_hbm, c_ref), (x_hbm, x_ref), (wq_hbm, wq_ref), (wk_hbm, wk_ref), (wv_hbm, wv_ref))
    ):
        copy = pltpu.make_async_copy(src, dst, load.at[n])
        copy.start()
        loads.append(copy)

    peers = [mate(k) for k in range(1, H)] + [(seq, other)]
    peers += [(g * H + flip(r, bit), other) for bit in BITS]
    for d in range(1, ng):
        far = (g + d) % ng
        peers += [(far * H + r, core), (far * H + mirror, core)]
    barrier = pltpu.get_barrier_semaphore()
    for peer in peers:
        pl.semaphore_signal(barrier, inc=1, device_id=peer, device_id_type=MESH)

    cut = 2 * DK + DV
    loads[0].wait()
    for h in range(H):
        own[h, cut:, :] = c_ref[:, h * DV : (h + 1) * DV].astype(F32).T
    pl.semaphore_wait(barrier, len(peers))
    ups = []
    for k in range(1, H):
        src = own.at[flip(r, k), pl.ds(cut, DV)]
        ups.append(push(src, rec.at[r, pl.ds(cut, DV)], us.at[k], ur.at[k], mate(k)))
    loads[1].wait()
    x = x_ref[...]
    for n, w_ref in enumerate((wq_ref, wk_ref)):
        loads[2 + n].wait()
        flat = dot(x, w_ref[...], (1, 0)).T
        for h in range(H):
            own[h, n * DK : (n + 1) * DK, :] = flat[h * DK : (h + 1) * DK]
    loads[4].wait()
    for h in range(H):
        own[h, 2 * DK : cut, :] = dot(x, wv_ref[:, h * DV : (h + 1) * DV], (1, 0)).T
    qkv = []
    for k in range(1, H):
        src = own.at[flip(r, k), pl.ds(0, cut)]
        qkv.append(push(src, rec.at[r, pl.ds(0, cut)], qs.at[k], qr.at[k], mate(k)))
    rec[r] = own[r]

    for cls in range(PLANE):
        for a in range(slots):
            at = ((a // 2) * H + cls + PLANE * (a % 2)) * owned
            st[cls, :, a * owned : (a + 1) * owned] = x_ref[:, at : at + owned].astype(F32)
    shares = []
    for k in range(1, PLANE):
        src = st.at[flip(r, k) % PLANE]
        shares.append(push(src, xg.at[r], xs.at[k], xr.at[k], mate(k)))
    xg[r] = st[r % PLANE]

    def lift(k):
        at = flip(r, k)
        return push(xg.at[at], xg.at[at], zs.at[k], zr.at[k], mate(PLANE))

    causal = lax.broadcasted_iota(jnp.int32, (span, span), 0) <= lax.broadcasted_iota(
        jnp.int32, (span, span), 1
    )
    ones = (lax.broadcasted_iota(jnp.int32, (AUX, span), 0) == 0).astype(F32)
    first = lax.broadcasted_iota(jnp.int32, (AUX, span), 0) == 0

    def part(c, start, count):
        rows = slice(start, start + count)
        return jnp.concatenate([rec[2 * c, rows, :], rec[2 * c + 1, rows, :]], 1)

    def relay(src, dst, send, recv, sign):
        for d in range(1, ng):
            to = g + sign * d

            @pl.when((to >= 0) & (to < ng))
            def _():
                push(src, dst.at[d], send.at[d], recv.at[d], (to * H + r, core))

    def settle(src, dst, send, recv, sign):
        for d in range(1, ng):
            to = g + sign * d

            @pl.when((to >= 0) & (to < ng))
            def _():
                pltpu.make_async_remote_copy(
                    src, dst.at[d], send.at[d], recv.at[d], (to * H + r, core), MESH
                ).wait_send()

    def collect(src, dst, send, recv, sign, total):
        total[...] = jnp.zeros(total.shape, F32)
        for d in range(1, ng):
            frm = g - sign * d

            @pl.when((frm >= 0) & (frm < ng))
            def _():
                pltpu.make_async_remote_copy(
                    src, dst.at[d], send.at[d], recv.at[d], (frm * H + r, core), MESH
                ).wait_recv()
                total[...] += dst[d]

    for copy in ups + qkv:
        copy.wait_recv()

    values = jnp.zeros((FEATS, DV), F32)
    norms = jnp.zeros((AUX, FEATS), F32)
    norm_at = []
    for c in range(chunks):
        fq = phi(part(c, 0, DK) * 0.5).astype(BF)
        fk = phi(part(c, DK, DK) * 0.5).astype(BF)
        va = jnp.concatenate([part(c, 2 * DK, DV), ones], 0).astype(BF)
        fqs[c] = fq
        fks[c] = fk
        vas[c] = va
        pv[c] = values
        norm_at.append(norms)
        values = values + dot(fk, va[:DV], (1, 1))
        norms = norms + dot(va[DV:], fk, (1, 1))
    ssend[...] = pack(values, norms)
    relay(ssend, srecv, ss, sr, 1)
    lifts = [lift(0)]

    for c in range(chunks):
        fq, fk, va = fqs[c], fks[c], vas[c]
        attn = halves(jnp.where(causal, dot(fk, fq, (0, 0)), 0.0))
        ah[c] = attn[0]
        al[c] = attn[1]
        top = dot2r(va, attn, (1, 0))
        if c > 0:
            top = top + jnp.concatenate(
                [dot2(halves(pv[c]), fq, (0, 0)), dot2(halves(norm_at[c]), fq, (1, 0))], 0
            )
        tops[c] = top

    collect(ssend, srecv, ss, sr, 1, sin)
    in_values, in_norms = unpack(sin[...])
    in_pair, in_norm_pair = halves(in_values), halves(in_norms)
    back = jnp.zeros((FEATS, DV), F32)
    back_norm = jnp.zeros((AUX, FEATS), F32)
    back_norm_at = [None] * chunks
    for c in reversed(range(chunks)):
        fq = fqs[c]
        top = tops[c] + jnp.concatenate(
            [dot2(in_pair, fq, (0, 0)), dot2(in_norm_pair, fq, (1, 0))], 0
        )
        scale = 1.0 / top[DV : DV + 1]
        numer = part(c, cut, DV) * scale
        denom = -jnp.sum(numer * top[:DV], 0, keepdims=True) * scale
        gn = halves(jnp.concatenate([numer, jnp.where(first, denom, 0.0)], 0))
        nh[c] = gn[0]
        nl[c] = gn[1]
        rv[c] = back
        back_norm_at[c] = back_norm
        back = back + dot2r(fq, (gn[0][:DV], gn[1][:DV]), (1, 1))
        back_norm = back_norm + dot2((gn[0][DV:], gn[1][DV:]), fq, (1, 1))
    rsend[...] = pack(back, back_norm)
    relay(rsend, rrecv, rs, rr, -1)
    shares[0].wait_recv()
    lifts.append(lift(1))

    def store(c, start, rows):
        half = 0 if start < HALF else 1
        at = start - half * HALF
        for b in range(2):
            o[2 * c + b, half, at : at + rows.shape[0], :] = rows[:, b * length : (b + 1) * length]

    for c in range(chunks):
        fq, fk, va = fqs[c], fks[c], vas[c]
        attn = (ah[c], al[c])
        gn = (nh[c], nl[c])
        ga = halves(jnp.where(causal, dot2r(va, gn, (0, 0)), 0.0))
        held = halves(pv[c] + in_values)
        held_norm = halves(norm_at[c] + in_norms)
        gfq = dot2r(fk, ga, (1, 0))
        gfq = gfq + dot3(held, (gn[0][:DV], gn[1][:DV]), (1, 0))
        gfq = gfq + dot3(held_norm, (gn[0][DV:], gn[1][DV:]), (0, 0))
        store(c, 0, pull(part(c, 0, DK) * 0.5, gfq) * 0.5)
        gv = dot3((gn[0][:DV], gn[1][:DV]), attn, (1, 1))
        gfk = dot2r(fq, ga, (1, 1))
        if c < chunks - 1:
            after = halves(rv[c])
            gv = gv + dot2(after, fk, (0, 0))
            gfk = gfk + dot2(after, va[:DV], (1, 0))
            gfk = gfk + dot2(halves(back_norm_at[c]), va[DV:], (0, 0))
        gvs[c] = gv
        gfks[c] = gfk

    for k in range(2, PLANE):
        shares[k - 1].wait_recv()
        lifts.append(lift(k))
    base = (r // PLANE) * PLANE
    near = push(
        xg.at[pl.ds(base, PLANE)], xp.at[pl.ds(base, PLANE)], ps.at[0], pr.at[0], (seq, other)
    )

    collect(rsend, rrecv, rs, rr, -1, rin)
    in_values, in_norms = unpack(rin[...])
    in_pair, in_norm_pair = halves(in_values), halves(in_norms)
    for c in range(chunks):
        fk, va = fks[c], vas[c]
        gv = gvs[c] + dot2(in_pair, fk, (0, 0))
        gfk = gfks[c] + dot2(in_pair, va[:DV], (1, 0)) + dot2(in_norm_pair, va[DV:], (0, 0))
        store(c, DK, gv[: DV // 2])
        store(c, HALF + DK, gv[DV // 2 :])
        store(c, HALF, pull(part(c, DK, DK) * 0.5, gfk) * 0.5)

    pending = [near] + shares + ups + qkv

    def direct(i):
        rows = pl.ds(i * ROWS, ROWS)
        for k in (1, 2):
            for half in range(2):
                pending.append(
                    push(
                        o.at[:, half, rows], gj.at[i, k, core], gs.at[i, k, half],
                        gr.at[i, k, core], (g * H + flip(r, k), half),
                    )
                )
        pending.append(
            push(
                o.at[:, other, rows], gj.at[i, 0, core], gs.at[i, 0, 0],
                gr.at[i, 0, core], (seq, other),
            )
        )

    def arrive(i, k, b):
        pltpu.make_async_copy(gj.at[i, k, b], gj.at[i, k, b], gr.at[i, k, b]).wait()

    def forward(i):
        k = 1 + i % 2
        for b in range(2):
            arrive(i, k, b)
        for b in range(2):
            pending.append(
                push(
                    gj.at[i, k, b], gj.at[i, PLANE - 1, b], hs.at[i, b],
                    gr.at[i, PLANE - 1, b], mate(PLANE - 1 - k),
                )
            )

    direct(0)
    direct(1)
    for i in range(PIECES):
        gj[i, 0, core] = o[:, core, i * ROWS : (i + 1) * ROWS, :]
    near.wait_recv()
    for j in range(PLANE):
        at = base + j
        rows = pl.ds(pl.multiple_of(at * length, length), length)
        xb[core, rows, :] = xg[at].astype(BF)
        xb[other, rows, :] = xp[at].astype(BF)
    forward(0)
    direct(2)
    for k in range(PLANE):
        lifts[k].wait_recv()
        at = flip(mirror, k)
        pending.append(push(xg.at[at], xp.at[at], ps.at[1 + k], pr.at[1 + k], (seq, other)))
    for k in range(PLANE):
        at = flip(mirror, k)
        rows = pl.ds(pl.multiple_of(at * length, length), length)
        xb[core, rows, :] = xg[at].astype(BF)
    for k in range(PLANE):
        pending[k - PLANE].wait_recv()
        at = flip(mirror, k)
        rows = pl.ds(pl.multiple_of(at * length, length), length)
        xb[other, rows, :] = xp[at].astype(BF)
    pending += lifts

    tokens = 2 * H * length
    sent = []
    for i in range(PIECES):
        if i + 1 < PIECES:
            forward(i + 1)
            if i + 3 < PIECES:
                direct(i + 3)
        for b in range(2):
            arrive(i, 2 - i % 2, b)
            arrive(i, PLANE - 1, b)
        arrive(i, 0, other)
        pending.append(
            push(
                gj.at[i, :, other, r], rt.at[0, core, i], ts.at[0, i, 0], tr.at[0, i, 0],
                (seq, other),
            )
        )
        for b in range(2):
            pending.append(
                push(
                    gj.at[i, :, b, mirror], rt.at[1, core, i], ts.at[1, i, b],
                    tr.at[1, i, core], (g * H + mirror, b),
                )
            )
        rt[0, core, i] = gj[i, :, core, r]
        rows = []
        for k in range(PLANE):
            rows.append(
                jnp.concatenate([gj[i, k, b, j] for b in range(2) for j in range(H)], 1)
            )
        grads = jnp.concatenate(rows, 0).astype(BF)
        product = dot(grads, xb[...].reshape(tokens, slots * owned), (1, 0))
        for a in range(slots):
            ls[i, a] = product[:, a * owned : (a + 1) * owned]
        row = []
        for d in range(ng):
            for w in range(2):
                if d == 0 and w == 0:
                    continue
                group = (g + d) % ng
                rank = r if w == 0 else mirror
                slot = group * 2 + rank // PLANE
                row.append(
                    push(
                        ls.at[i, slot], lr.at[i, d, w], bs.at[i, d, w], br.at[i, d, w],
                        (group * H + rank, core),
                    )
                )
        sent.append(row)

    for i in range(PIECES):
        pltpu.make_async_copy(rt.at[0, other, i], rt.at[0, other, i], tr.at[0, i, 0]).wait()
        for b in range(2):
            pltpu.make_async_copy(rt.at[1, b, i], rt.at[1, b, i], tr.at[1, i, b]).wait()

    def back_rows(h, half):
        low = [((h // bit + r // bit) % 2) * bit for bit in (1, 2)]
        place = (h // PLANE + r // PLANE) % 2
        return jnp.concatenate([rt[place, half, i, low[0] + low[1]] for i in range(PIECES)], 0)

    whole = [[back_rows(h, half) for half in range(2)] for h in range(H)]
    blocks = [jnp.concatenate([whole[h][n][:DK] for h in range(H)], 0) for n in range(2)]
    for h in range(H):
        blocks.append(jnp.concatenate([whole[h][0][DK:], whole[h][1][DK:]], 0))
    for n, block in enumerate(blocks):
        jt[:, n * DV : (n + 1) * DV] = block.T.astype(BF)
    step = 512
    for at in range(0, width, step):
        rows = slice(at, at + step)
        total = dot(jt[:, :DV], wq_ref[rows, :], (1, 1))
        total = total + dot(jt[:, DV : 2 * DV], wk_ref[rows, :], (1, 1))
        total = total + dot(jt[:, 2 * DV :], wv_ref[rows, :], (1, 1))
        gi_ref[:, rows] = total.astype(BF)

    swaps = []
    for i in range(PIECES):
        for copy in sent[i]:
            copy.wait_recv()
        mine = ls[i, g * 2 + r // PLANE]
        rest = lr[i, 0, 1]
        for d in range(1, ng):
            mine = mine + lr[i, d, 0]
            rest = rest + lr[i, d, 1]
        for k in range(PLANE):
            f2[core, i, flip(r, k)] = mine[k * ROWS : (k + 1) * ROWS]
            f2[core, i, flip(mirror, k)] = rest[k * ROWS : (k + 1) * ROWS]
        swaps.append(push(f2.at[core, i], f2.at[core, i], ds.at[i], dr.at[i], (seq, other)))
    for copy in swaps:
        copy.wait_recv()
    final = [jnp.concatenate([f2[n, 0, h, :DK] for h in range(H)], 0) for n in range(2)]
    for h in range(H):
        parts = []
        for n in range(2):
            for i in range(PIECES):
                start = max(DK - i * ROWS, 0)
                if start < ROWS:
                    parts.append(f2[n, i, h, start:])
        final.append(jnp.concatenate(parts, 0))
    keep = owned // 2
    for n, block in enumerate(final):
        fs[n] = block.T
        out_ref[n] = fs[n, pl.ds(pl.multiple_of(core * keep, keep), keep), :]
    pending += swaps
    for row in sent:
        pending += row
    for copy in pending:
        copy.wait_send()
    settle(ssend, srecv, ss, sr, 1)
    settle(rsend, rrecv, rs, rr, -1)


def fused(tokens, upstream, weights, ng):
    length, width = tokens.shape
    owned = width // (ng * H)
    slots = 2 * ng
    chunks, span = H // 2, 2 * length
    vm = lambda *shape: pltpu.VMEM(shape, F32)
    half = lambda *shape: pltpu.VMEM(shape, BF)
    state = (FEATS + 16, DV)
    scratch = [half(length, width), half(length, H * DV)]
    scratch += [pltpu.VMEM(w.shape, w.dtype) for w in weights]
    scratch += [
        vm(H, 2 * DK + 2 * DV, length), vm(H, 2 * DK + 2 * DV, length),
        vm(PLANE, length, slots * owned), vm(H, length, slots * owned),
        vm(H, length, slots * owned), half(2, H * length, slots * owned),
        half(chunks, FEATS, span), half(chunks, FEATS, span), half(chunks, DV + AUX, span),
        half(chunks, span, span), half(chunks, span, span),
        half(chunks, DV + AUX, span), half(chunks, DV + AUX, span),
        vm(chunks, DV + AUX, span), vm(chunks, FEATS, DV), vm(chunks, FEATS, DV),
        vm(chunks, DV, span), vm(chunks, FEATS, span),
        vm(*state), vm(ng, *state), vm(*state), vm(*state), vm(ng, *state), vm(*state),
        vm(H, 2, HALF, length), vm(PIECES, PLANE, 2, H, ROWS, length),
        vm(PIECES, slots, PLANE * ROWS, owned), vm(PIECES, ng, 2, PLANE * ROWS, owned),
        vm(2, 2, PIECES, PLANE, ROWS, length), half(length, H * DV + 2 * DV),
        vm(2, PIECES, H, ROWS, owned), vm(2 + H, owned, DV),
        sems(5),
        sems(H), sems(H), sems(H), sems(H), sems(PLANE), sems(PLANE), sems(PLANE), sems(PLANE),
        sems(1 + PLANE), sems(1 + PLANE), sems(ng), sems(ng), sems(ng), sems(ng),
        sems(PIECES, PLANE, 2), sems(PIECES, PLANE, 2), sems(PIECES, 2),
        sems(2, PIECES, 2), sems(2, PIECES, 2),
        sems(PIECES, ng, 2), sems(PIECES, ng, 2), sems(PIECES), sems(PIECES),
    ]
    return pl.pallas_call(
        functools.partial(fused_kernel, ng),
        out_shape=[
            jax.ShapeDtypeStruct((length, width), BF),
            jax.ShapeDtypeStruct((2 + H, owned // 2, DV), F32),
        ],
        in_specs=[HBM] * 5,
        out_specs=[VMEM] * 2,
        scratch_shapes=scratch,
        compiler_params=pltpu.CompilerParams(
            collective_id=0, has_side_effects=True, vmem_limit_bytes=60 << 20
        ),
    )(tokens, upstream, *weights)


def finish_kernel(gi_ref, o_ref, in_ref, oq_ref, ok_ref, ov_ref):
    in_ref[0] = gi_ref[...]
    oq_ref[...] = o_ref[0]
    ok_ref[...] = o_ref[1]
    for n in range(H):
        ov_ref[:, n * DV : (n + 1) * DV] = o_ref[2 + n]


def finish(grad_in, blocks):
    _, rows, lanes = blocks.shape
    return pl.pallas_call(
        finish_kernel,
        out_shape=[
            jax.ShapeDtypeStruct((1,) + grad_in.shape, BF),
            jax.ShapeDtypeStruct((rows, lanes), F32),
            jax.ShapeDtypeStruct((rows, lanes), F32),
            jax.ShapeDtypeStruct((rows, H * lanes), F32),
        ],
        in_specs=[VMEM] * 2,
        out_specs=[VMEM] * 4,
    )(grad_in, blocks)


def body(inputs, cotangent, w_query, w_key, w_value):
    ng = lax.axis_size("seq") // H
    weights = (w_query, w_key, w_value)
    return tuple(finish(*fused(inputs[0], cotangent[0], weights, ng)))


def solution(mesh):
    in_specs = (P("batch", "seq", None), P("batch", "seq", None), P(), P(), P())
    out_specs = (
        P("batch", "seq", None),
        P(("seq", "batch"), None),
        P(("seq", "batch"), None),
        P(("seq", "batch"), None),
    )
    return jax.shard_map(body, mesh=mesh, in_specs=in_specs, out_specs=out_specs, check_vma=False)
```

```python
import functools
import math

import jax
import jax.numpy as jnp
from jax import lax
from jax.experimental import pallas as pl
from jax.experimental.pallas import tpu as pltpu
from jax.sharding import PartitionSpec as P

H = 8
DK = 16
DV = 128
AUX = 16
PAIRS = DK * (DK + 1) // 2
FEATS = PAIRS + DK + 8
HALF = DK + DV // 2
PIECES = 5
ROWS = HALF // PIECES
BITS = (1, 2, 4)
PLANE = 4
MESH = pl.DeviceIdType.MESH
BF = jnp.bfloat16
F32 = jnp.float32
VMEM = pl.BlockSpec(memory_space=pltpu.VMEM)
HBM = pl.BlockSpec(memory_space=pl.ANY)


def push(src, dst, send, recv, device):
    copy = pltpu.make_async_remote_copy(
        src_ref=src,
        dst_ref=dst,
        send_sem=send,
        recv_sem=recv,
        device_id=device,
        device_id_type=MESH,
    )
    copy.start()
    return copy


def sems(*sizes):
    return pltpu.SemaphoreType.DMA(sizes)


def dot(left, right, dims):
    return lax.dot_general(left, right, ((dims[:1], dims[1:]), ((), ())), preferred_element_type=F32)


def halves(a):
    high = a.astype(BF)
    return high, (a - high.astype(F32)).astype(BF)


def dot2(pair, right, dims):
    return dot(pair[0], right, dims) + dot(pair[1], right, dims)


def dot2r(left, pair, dims):
    return dot(left, pair[0], dims) + dot(left, pair[1], dims)


def dot3(lefts, rights, dims):
    return (
        dot(lefts[0], rights[0], dims)
        + dot(lefts[0], rights[1], dims)
        + dot(lefts[1], rights[0], dims)
    )


def flip(rank, mask):
    for bit in BITS:
        if mask & bit:
            rank = rank + bit - 2 * bit * ((rank // bit) % 2)
    return rank


def phi(u):
    half = DK // 2
    lanes = u.shape[1]
    pieces = [u * u * math.sqrt(0.5)]
    for s in range(1, half):
        pieces.append(u * pltpu.roll(u, DK - s, 0))
    pieces.append(u[:half] * u[half:])
    pieces.append(u)
    pieces.append((lax.broadcasted_iota(jnp.int32, (8, lanes), 0) == 0).astype(F32))
    return jnp.concatenate(pieces, 0)


def pull(u, grad):
    half = DK // 2
    total = grad[PAIRS : PAIRS + DK] + grad[:DK] * u * math.sqrt(2.0)
    for s in range(1, half):
        piece = grad[s * DK : (s + 1) * DK]
        total = total + piece * pltpu.roll(u, DK - s, 0) + pltpu.roll(piece * u, s, 0)
    last = grad[half * DK : half * DK + half]
    return total + jnp.concatenate([last * u[half:], last * u[:half]], 0)


def pack(values, norms):
    low = norms[:8, :DV]
    high = jnp.concatenate([norms[:8, DV:], jnp.zeros((8, 2 * DV - FEATS), F32)], 1)
    return jnp.concatenate([values, low, high], 0)


def unpack(packed):
    values = packed[:FEATS]
    norms = jnp.concatenate([packed[FEATS : FEATS + 8], packed[FEATS + 8 :, : FEATS - DV]], 1)
    return values, jnp.concatenate([norms, jnp.zeros((AUX - 8, FEATS), F32)], 0)


def fused_kernel(
    ng, x_hbm, c_hbm, wq_hbm, wk_hbm, wv_hbm, gi_ref, out_ref,
    x_ref, c_ref, wq_ref, wk_ref, wv_ref, own, rec, st, xg, xp, xb,
    fqs, fks, vas, ah, al, nh, nl, tops, pv, rv, gvs, gfks,
    ssend, srecv, sin, rsend, rrecv, rin, o, gj, ls, lr, acc, l2, rt, jt, f2, fs,
    load, us, ur, qs, qr, xs, xr, ps, pr, ss, sr, rs, rr,
    zs, gs, gr, hs, ts, tr, bs, br, cs, cr, ds, dr,
):
    seq = lax.axis_index("seq")
    core = lax.axis_index("batch")
    other = 1 - core
    g = seq // H
    r = seq % H
    mirror = flip(r, PLANE)
    length = x_ref.shape[0]
    width = x_ref.shape[1]
    owned = width // (ng * H)
    slots = 2 * ng
    chunks = H // 2
    span = 2 * length

    def mate(k):
        return (g * H + flip(r, k), core)

    loads = []
    for n, (src, dst) in enumerate(
        ((c_hbm, c_ref), (x_hbm, x_ref), (wq_hbm, wq_ref), (wk_hbm, wk_ref), (wv_hbm, wv_ref))
    ):
        copy = pltpu.make_async_copy(src, dst, load.at[n])
        copy.start()
        loads.append(copy)

    peers = [mate(k) for k in range(1, H)] + [(seq, other)]
    peers += [(g * H + flip(r, bit), other) for bit in BITS]
    for d in range(1, ng):
        far = (g + d) % ng
        peers.append((far * H + r, core))
    barrier = pltpu.get_barrier_semaphore()
    for peer in peers:
        pl.semaphore_signal(barrier, inc=1, device_id=peer, device_id_type=MESH)

    cut = 2 * DK + DV
    loads[0].wait()
    for h in range(H):
        own[h, cut:, :] = c_ref[:, h * DV : (h + 1) * DV].astype(F32).T
    pl.semaphore_wait(barrier, len(peers))
    ups = []
    for k in range(1, H):
        src = own.at[flip(r, k), pl.ds(cut, DV)]
        ups.append(push(src, rec.at[r, pl.ds(cut, DV)], us.at[k], ur.at[k], mate(k)))
    loads[1].wait()
    x = x_ref[...]
    for n, w_ref in enumerate((wq_ref, wk_ref)):
        loads[2 + n].wait()
        flat = dot(x, w_ref[...], (1, 0)).T
        for h in range(H):
            own[h, n * DK : (n + 1) * DK, :] = flat[h * DK : (h + 1) * DK]
    loads[4].wait()
    for h in range(H):
        own[h, 2 * DK : cut, :] = dot(x, wv_ref[:, h * DV : (h + 1) * DV], (1, 0)).T
    qkv = []
    for k in range(1, H):
        src = own.at[flip(r, k), pl.ds(0, cut)]
        qkv.append(push(src, rec.at[r, pl.ds(0, cut)], qs.at[k], qr.at[k], mate(k)))
    rec[r] = own[r]

    for cls in range(PLANE):
        for a in range(slots):
            at = ((a // 2) * H + cls + PLANE * (a % 2)) * owned
            st[cls, :, a * owned : (a + 1) * owned] = x_ref[:, at : at + owned].astype(F32)
    shares = []
    for k in range(1, PLANE):
        src = st.at[flip(r, k) % PLANE]
        shares.append(push(src, xg.at[r], xs.at[k], xr.at[k], mate(k)))
    xg[r] = st[r % PLANE]

    causal = lax.broadcasted_iota(jnp.int32, (span, span), 0) <= lax.broadcasted_iota(
        jnp.int32, (span, span), 1
    )
    ones = (lax.broadcasted_iota(jnp.int32, (AUX, span), 0) == 0).astype(F32)
    first = lax.broadcasted_iota(jnp.int32, (AUX, span), 0) == 0

    def part(c, start, count):
        rows = slice(start, start + count)
        return jnp.concatenate([rec[2 * c, rows, :], rec[2 * c + 1, rows, :]], 1)

    def relay(src, dst, send, recv, sign):
        for d in range(1, ng):
            to = g + sign * d

            @pl.when((to >= 0) & (to < ng))
            def _():
                push(src, dst.at[d], send.at[d], recv.at[d], (to * H + r, core))

    def settle(src, dst, send, recv, sign):
        for d in range(1, ng):
            to = g + sign * d

            @pl.when((to >= 0) & (to < ng))
            def _():
                pltpu.make_async_remote_copy(
                    src, dst.at[d], send.at[d], recv.at[d], (to * H + r, core), MESH
                ).wait_send()

    def collect(src, dst, send, recv, sign, total):
        total[...] = jnp.zeros(total.shape, F32)
        for d in range(1, ng):
            frm = g - sign * d

            @pl.when((frm >= 0) & (frm < ng))
            def _():
                pltpu.make_async_remote_copy(
                    src, dst.at[d], send.at[d], recv.at[d], (frm * H + r, core), MESH
                ).wait_recv()
                total[...] += dst[d]

    for copy in ups + qkv:
        copy.wait_recv()

    values = jnp.zeros((FEATS, DV), F32)
    norms = jnp.zeros((AUX, FEATS), F32)
    norm_at = []
    for c in range(chunks):
        fq = phi(part(c, 0, DK) * 0.5).astype(BF)
        fk = phi(part(c, DK, DK) * 0.5).astype(BF)
        va = jnp.concatenate([part(c, 2 * DK, DV), ones], 0).astype(BF)
        fqs[c] = fq
        fks[c] = fk
        vas[c] = va
        pv[c] = values
        norm_at.append(norms)
        values = values + dot(fk, va[:DV], (1, 1))
        norms = norms + dot(va[DV:], fk, (1, 1))
    ssend[...] = pack(values, norms)
    relay(ssend, srecv, ss, sr, 1)

    for c in range(chunks):
        fq, fk, va = fqs[c], fks[c], vas[c]
        attn = halves(jnp.where(causal, dot(fk, fq, (0, 0)), 0.0))
        ah[c] = attn[0]
        al[c] = attn[1]
        top = dot2r(va, attn, (1, 0))
        if c > 0:
            top = top + jnp.concatenate(
                [dot2(halves(pv[c]), fq, (0, 0)), dot2(halves(norm_at[c]), fq, (1, 0))], 0
            )
        tops[c] = top

    collect(ssend, srecv, ss, sr, 1, sin)
    in_values, in_norms = unpack(sin[...])
    in_pair, in_norm_pair = halves(in_values), halves(in_norms)
    back = jnp.zeros((FEATS, DV), F32)
    back_norm = jnp.zeros((AUX, FEATS), F32)
    back_norm_at = [None] * chunks
    for c in reversed(range(chunks)):
        fq = fqs[c]
        top = tops[c] + jnp.concatenate(
            [dot2(in_pair, fq, (0, 0)), dot2(in_norm_pair, fq, (1, 0))], 0
        )
        scale = 1.0 / top[DV : DV + 1]
        numer = part(c, cut, DV) * scale
        denom = -jnp.sum(numer * top[:DV], 0, keepdims=True) * scale
        gn = halves(jnp.concatenate([numer, jnp.where(first, denom, 0.0)], 0))
        nh[c] = gn[0]
        nl[c] = gn[1]
        rv[c] = back
        back_norm_at[c] = back_norm
        back = back + dot2r(fq, (gn[0][:DV], gn[1][:DV]), (1, 1))
        back_norm = back_norm + dot2((gn[0][DV:], gn[1][DV:]), fq, (1, 1))
    rsend[...] = pack(back, back_norm)
    relay(rsend, rrecv, rs, rr, -1)
    def store(c, start, rows):
        half = 0 if start < HALF else 1
        at = start - half * HALF
        for b in range(2):
            o[2 * c + b, half, at : at + rows.shape[0], :] = rows[:, b * length : (b + 1) * length]

    for c in range(chunks):
        fq, fk, va = fqs[c], fks[c], vas[c]
        attn = (ah[c], al[c])
        gn = (nh[c], nl[c])
        ga = halves(jnp.where(causal, dot2r(va, gn, (0, 0)), 0.0))
        held = halves(pv[c] + in_values)
        held_norm = halves(norm_at[c] + in_norms)
        gfq = dot2r(fk, ga, (1, 0))
        gfq = gfq + dot3(held, (gn[0][:DV], gn[1][:DV]), (1, 0))
        gfq = gfq + dot3(held_norm, (gn[0][DV:], gn[1][DV:]), (0, 0))
        store(c, 0, pull(part(c, 0, DK) * 0.5, gfq) * 0.5)
        gv = dot3((gn[0][:DV], gn[1][:DV]), attn, (1, 1))
        gfk = dot2r(fq, ga, (1, 1))
        if c < chunks - 1:
            after = halves(rv[c])
            gv = gv + dot2(after, fk, (0, 0))
            gfk = gfk + dot2(after, va[:DV], (1, 0))
            gfk = gfk + dot2(halves(back_norm_at[c]), va[DV:], (0, 0))
        gvs[c] = gv
        gfks[c] = gfk

    for copy in shares:
        copy.wait_recv()
    base = (r // PLANE) * PLANE
    near = push(
        xg.at[pl.ds(base, PLANE)], xp.at[pl.ds(base, PLANE)], ps.at[0], pr.at[0], (seq, other)
    )

    collect(rsend, rrecv, rs, rr, -1, rin)
    in_values, in_norms = unpack(rin[...])
    in_pair, in_norm_pair = halves(in_values), halves(in_norms)
    for c in range(chunks):
        fk, va = fks[c], vas[c]
        gv = gvs[c] + dot2(in_pair, fk, (0, 0))
        gfk = gfks[c] + dot2(in_pair, va[:DV], (1, 0)) + dot2(in_norm_pair, va[DV:], (0, 0))
        store(c, DK, gv[: DV // 2])
        store(c, HALF + DK, gv[DV // 2 :])
        store(c, HALF, pull(part(c, DK, DK) * 0.5, gfk) * 0.5)

    pending = [near] + shares + ups + qkv
    here = pl.ds(base, PLANE)
    there = pl.ds(PLANE - base, PLANE)
    place = r % PLANE
    side = r // PLANE

    def across(i):
        rows = pl.ds(i * ROWS, ROWS)
        for half in range(2):
            pending.append(
                push(
                    o.at[there, half, rows], gj.at[i, 1, 0, core], zs.at[i, half],
                    gr.at[i, 1, 0, core], (g * H + mirror, half),
                )
            )

    def direct(i):
        rows = pl.ds(i * ROWS, ROWS)
        for k in (1, 2):
            for half in range(2):
                pending.append(
                    push(
                        o.at[here, half, rows], gj.at[i, 0, k, core], gs.at[i, 0, k, half],
                        gr.at[i, 0, k, core], (g * H + flip(r, k), half),
                    )
                )
        pending.append(
            push(
                o.at[here, other, rows], gj.at[i, 0, 0, core], gs.at[i, 0, 0, 0],
                gr.at[i, 0, 0, core], (seq, other),
            )
        )

    def landed(ref, sem):
        pltpu.make_async_copy(ref, ref, sem).wait()

    def arrive(i, m, k):
        if m == 0 or k == 0:
            if k < PLANE - 1:
                for b in range(2):
                    landed(gj.at[i, m, k, b], gr.at[i, m, k, b])
                return
        landed(gj.at[i, m, k], gr.at[i, m, k, 0])

    def mirrored(i):
        arrive(i, 1, 0)
        for k in (1, 2):
            pending.append(
                push(
                    gj.at[i, 1, 0], gj.at[i, 1, k], gs.at[i, 1, k, 0], gr.at[i, 1, k, 0], mate(k)
                )
            )

    def turn(i, m):
        return 1 + (i + m) % 2

    def forward(i, m):
        k = turn(i, m)
        arrive(i, m, k)
        pending.append(
            push(
                gj.at[i, m, k], gj.at[i, m, PLANE - 1], hs.at[i, m],
                gr.at[i, m, PLANE - 1, 0], mate(PLANE - 1 - k),
            )
        )

    def multiply(i, m):
        arrive(i, m, PLANE - 1 - turn(i, m))
        arrive(i, m, PLANE - 1)
        if m == 0:
            landed(gj.at[i, 0, 0, other], gr.at[i, 0, 0, other])
        pending.append(
            push(
                gj.at[i, m, :, other, place], rt.at[core, i, m], ts.at[i, m], tr.at[i, m],
                (seq, other),
            )
        )
        rt[core, i, m] = gj[i, m, :, core, place]
        rows = []
        for k in range(PLANE):
            rows.append(
                jnp.concatenate([gj[i, m, k, b, j] for b in range(2) for j in range(PLANE)], 1)
            )
        grads = jnp.concatenate(rows, 0).astype(BF)
        product = dot(grads, xb[...].reshape(2 * PLANE * length, slots * owned), (1, 0))
        for a in range(slots):
            ls[i, m, a % 2, a // 2] = product[:, a * owned : (a + 1) * owned]
        pending.append(
            push(
                ls.at[i, m, 1 - side], lr.at[i, 1 - m], bs.at[i, m], br.at[i, 1 - m], mate(PLANE)
            )
        )

    def combine(i):
        for m in range(2):
            landed(lr.at[i, m], br.at[i, m])
            for a in range(ng):
                acc[i, a, m] = ls[i, m, side, a] + lr[i, m, a]
        for d in range(1, ng):
            to = (g + d) % ng
            pending.append(
                push(acc.at[i, to], l2.at[i, d], cs.at[i, d], cr.at[i, d], (to * H + r, core))
            )

    swaps = []

    def settled(i):
        total = acc[i, g]
        for d in range(1, ng):
            landed(l2.at[i, d], cr.at[i, d])
            total = total + l2[i, d]
        for m in range(2):
            for k in range(PLANE):
                rows = total[m, k * ROWS : (k + 1) * ROWS]
                f2[core, i, flip(mirror if m else r, k)] = rows
        swaps.append(push(f2.at[core, i], f2.at[core, i], ds.at[i], dr.at[i], (seq, other)))

    across(0)
    direct(0)
    across(1)
    direct(1)
    for i in range(2, PIECES):
        across(i)
    for i in range(PIECES):
        gj[i, 0, 0, core] = o[here, core, i * ROWS : (i + 1) * ROWS, :]
    near.wait_recv()
    for j in range(PLANE):
        xb[core, j * length : (j + 1) * length, :] = xg[base + j].astype(BF)
        xb[other, j * length : (j + 1) * length, :] = xp[base + j].astype(BF)
    mirrored(0)
    forward(0, 0)
    for i in range(PIECES):
        if i + 1 < PIECES:
            mirrored(i + 1)
            forward(i + 1, 0)
        if i + 2 < PIECES:
            direct(i + 2)
        forward(i, 1)
        multiply(i, 0)
        multiply(i, 1)
        if i > 0:
            combine(i - 1)
        if i > 1:
            settled(i - 2)
    for i in range(PIECES):
        for m in range(2):
            landed(rt.at[other, i, m], tr.at[i, m])

    def back_rows(h, half):
        low = [((h // bit + r // bit) % 2) * bit for bit in (1, 2)]
        m = (h // PLANE + r // PLANE) % 2
        return jnp.concatenate([rt[half, i, m, low[0] + low[1]] for i in range(PIECES)], 0)

    whole = [[back_rows(h, half) for half in range(2)] for h in range(H)]
    blocks = [jnp.concatenate([whole[h][n][:DK] for h in range(H)], 0) for n in range(2)]
    for h in range(H):
        blocks.append(jnp.concatenate([whole[h][0][DK:], whole[h][1][DK:]], 0))
    for n, block in enumerate(blocks):
        jt[:, n * DV : (n + 1) * DV] = block.T.astype(BF)
    step = 512
    for at in range(0, width, step):
        rows = slice(at, at + step)
        total = dot(jt[:, :DV], wq_ref[rows, :], (1, 1))
        total = total + dot(jt[:, DV : 2 * DV], wk_ref[rows, :], (1, 1))
        total = total + dot(jt[:, 2 * DV :], wv_ref[rows, :], (1, 1))
        gi_ref[:, rows] = total.astype(BF)

    combine(PIECES - 1)
    for i in range(PIECES - 2, PIECES):
        settled(i)
    for copy in swaps:
        copy.wait_recv()
    final = [jnp.concatenate([f2[n, 0, h, :DK] for h in range(H)], 0) for n in range(2)]
    for h in range(H):
        parts = []
        for n in range(2):
            for i in range(PIECES):
                start = max(DK - i * ROWS, 0)
                if start < ROWS:
                    parts.append(f2[n, i, h, start:])
        final.append(jnp.concatenate(parts, 0))
    keep = owned // 2
    for n, block in enumerate(final):
        fs[n] = block.T
        out_ref[n] = fs[n, pl.ds(pl.multiple_of(core * keep, keep), keep), :]
    pending += swaps
    for copy in pending:
        copy.wait_send()
    settle(ssend, srecv, ss, sr, 1)
    settle(rsend, rrecv, rs, rr, -1)


def fused(tokens, upstream, weights, ng):
    length, width = tokens.shape
    owned = width // (ng * H)
    slots = 2 * ng
    chunks, span = H // 2, 2 * length
    vm = lambda *shape: pltpu.VMEM(shape, F32)
    half = lambda *shape: pltpu.VMEM(shape, BF)
    state = (FEATS + 16, DV)
    scratch = [half(length, width), half(length, H * DV)]
    scratch += [pltpu.VMEM(w.shape, w.dtype) for w in weights]
    scratch += [
        vm(H, 2 * DK + 2 * DV, length), vm(H, 2 * DK + 2 * DV, length),
        vm(PLANE, length, slots * owned), vm(H, length, slots * owned),
        vm(H, length, slots * owned), half(2, PLANE * length, slots * owned),
        half(chunks, FEATS, span), half(chunks, FEATS, span), half(chunks, DV + AUX, span),
        half(chunks, span, span), half(chunks, span, span),
        half(chunks, DV + AUX, span), half(chunks, DV + AUX, span),
        vm(chunks, DV + AUX, span), vm(chunks, FEATS, DV), vm(chunks, FEATS, DV),
        vm(chunks, DV, span), vm(chunks, FEATS, span),
        vm(*state), vm(ng, *state), vm(*state), vm(*state), vm(ng, *state), vm(*state),
        vm(H, 2, HALF, length), vm(PIECES, 2, PLANE, 2, PLANE, ROWS, length),
        vm(PIECES, 2, 2, ng, PLANE * ROWS, owned), vm(PIECES, 2, ng, PLANE * ROWS, owned),
        vm(PIECES, ng, 2, PLANE * ROWS, owned), vm(PIECES, ng, 2, PLANE * ROWS, owned),
        vm(2, PIECES, 2, PLANE, ROWS, length), half(length, H * DV + 2 * DV),
        vm(2, PIECES, H, ROWS, owned), vm(2 + H, owned, DV),
        sems(5),
        sems(H), sems(H), sems(H), sems(H), sems(PLANE), sems(PLANE),
        sems(1), sems(1), sems(ng), sems(ng), sems(ng), sems(ng),
        sems(PIECES, 2), sems(PIECES, 2, PLANE, 2), sems(PIECES, 2, PLANE, 2), sems(PIECES, 2),
        sems(PIECES, 2), sems(PIECES, 2), sems(PIECES, 2), sems(PIECES, 2),
        sems(PIECES, ng), sems(PIECES, ng), sems(PIECES), sems(PIECES),
    ]
    return pl.pallas_call(
        functools.partial(fused_kernel, ng),
        out_shape=[
            jax.ShapeDtypeStruct((length, width), BF),
            jax.ShapeDtypeStruct((2 + H, owned // 2, DV), F32),
        ],
        in_specs=[HBM] * 5,
        out_specs=[VMEM] * 2,
        scratch_shapes=scratch,
        compiler_params=pltpu.CompilerParams(
            collective_id=0, has_side_effects=True, vmem_limit_bytes=60 << 20
        ),
    )(tokens, upstream, *weights)


def finish_kernel(gi_ref, o_ref, in_ref, oq_ref, ok_ref, ov_ref):
    in_ref[0] = gi_ref[...]
    oq_ref[...] = o_ref[0]
    ok_ref[...] = o_ref[1]
    for n in range(H):
        ov_ref[:, n * DV : (n + 1) * DV] = o_ref[2 + n]


def finish(grad_in, blocks):
    _, rows, lanes = blocks.shape
    return pl.pallas_call(
        finish_kernel,
        out_shape=[
            jax.ShapeDtypeStruct((1,) + grad_in.shape, BF),
            jax.ShapeDtypeStruct((rows, lanes), F32),
            jax.ShapeDtypeStruct((rows, lanes), F32),
            jax.ShapeDtypeStruct((rows, H * lanes), F32),
        ],
        in_specs=[VMEM] * 2,
        out_specs=[VMEM] * 4,
    )(grad_in, blocks)


def body(inputs, cotangent, w_query, w_key, w_value):
    ng = lax.axis_size("seq") // H
    weights = (w_query, w_key, w_value)
    return tuple(finish(*fused(inputs[0], cotangent[0], weights, ng)))


def solution(mesh):
    in_specs = (P("batch", "seq", None), P("batch", "seq", None), P(), P(), P())
    out_specs = (
        P("batch", "seq", None),
        P(("seq", "batch"), None),
        P(("seq", "batch"), None),
        P(("seq", "batch"), None),
    )
    return jax.shard_map(body, mesh=mesh, in_specs=in_specs, out_specs=out_specs, check_vma=False)
```

```python
import functools
import math

import jax
import jax.numpy as jnp
from jax import lax
from jax.experimental import pallas as pl
from jax.experimental.pallas import tpu as pltpu
from jax.sharding import PartitionSpec as P

H = 8
DK = 16
DV = 128
AUX = 16
PAIRS = DK * (DK + 1) // 2
FEATS = PAIRS + DK + 8
HALF = DK + DV // 2
PIECES = 5
ROWS = HALF // PIECES
BITS = (1, 2, 4)
PLANE = 4
LAGS = (0, 2, 4, 6, 8)
LEAD = 3
MESH = pl.DeviceIdType.MESH
BF = jnp.bfloat16
F32 = jnp.float32
VMEM = pl.BlockSpec(memory_space=pltpu.VMEM)
HBM = pl.BlockSpec(memory_space=pl.ANY)


def push(src, dst, send, recv, device):
    copy = pltpu.make_async_remote_copy(
        src_ref=src,
        dst_ref=dst,
        send_sem=send,
        recv_sem=recv,
        device_id=device,
        device_id_type=MESH,
    )
    copy.start()
    return copy


def sems(*sizes):
    return pltpu.SemaphoreType.DMA(sizes)


def dot(left, right, dims):
    return lax.dot_general(left, right, ((dims[:1], dims[1:]), ((), ())), preferred_element_type=F32)


def halves(a):
    high = a.astype(BF)
    return high, (a - high.astype(F32)).astype(BF)


def dot2(pair, right, dims):
    return dot(pair[0], right, dims) + dot(pair[1], right, dims)


def dot2r(left, pair, dims):
    return dot(left, pair[0], dims) + dot(left, pair[1], dims)


def dot3(lefts, rights, dims):
    return (
        dot(lefts[0], rights[0], dims)
        + dot(lefts[0], rights[1], dims)
        + dot(lefts[1], rights[0], dims)
    )


def flip(rank, mask):
    for bit in BITS:
        if mask & bit:
            rank = rank + bit - 2 * bit * ((rank // bit) % 2)
    return rank


def phi(u):
    half = DK // 2
    lanes = u.shape[1]
    pieces = [u * u * math.sqrt(0.5)]
    for s in range(1, half):
        pieces.append(u * pltpu.roll(u, DK - s, 0))
    pieces.append(u[:half] * u[half:])
    pieces.append(u)
    pieces.append((lax.broadcasted_iota(jnp.int32, (8, lanes), 0) == 0).astype(F32))
    return jnp.concatenate(pieces, 0)


def pull(u, grad):
    half = DK // 2
    total = grad[PAIRS : PAIRS + DK] + grad[:DK] * u * math.sqrt(2.0)
    for s in range(1, half):
        piece = grad[s * DK : (s + 1) * DK]
        total = total + piece * pltpu.roll(u, DK - s, 0) + pltpu.roll(piece * u, s, 0)
    last = grad[half * DK : half * DK + half]
    return total + jnp.concatenate([last * u[half:], last * u[:half]], 0)


def pack(values, norms):
    low = norms[:8, :DV]
    high = jnp.concatenate([norms[:8, DV:], jnp.zeros((8, 2 * DV - FEATS), F32)], 1)
    return jnp.concatenate([values, low, high], 0)


def unpack(packed):
    values = packed[:FEATS]
    norms = jnp.concatenate([packed[FEATS : FEATS + 8], packed[FEATS + 8 :, : FEATS - DV]], 1)
    return values, jnp.concatenate([norms, jnp.zeros((AUX - 8, FEATS), F32)], 0)


def fused_kernel(
    ng, x_hbm, c_hbm, wq_hbm, wk_hbm, wv_hbm, gi_ref, out_ref,
    x_ref, c_ref, wq_ref, wk_ref, wv_ref, own, rec, st, xg, xp, xb,
    fqs, fks, vas, ah, al, nh, nl, tops, pv, rv, gvs, gfks,
    ssend, srecv, sin, rsend, rrecv, rin, o, gj, ls, lr, acc, l2, rt, jt, f2, fs,
    load, us, ur, qs, qr, xs, xr, ps, pr, ss, sr, rs, rr,
    zs, gs, gr, hs, ts, tr, bs, br, cs, cr, ds, dr,
):
    seq = lax.axis_index("seq")
    core = lax.axis_index("batch")
    other = 1 - core
    g = seq // H
    r = seq % H
    mirror = flip(r, PLANE)
    length = x_ref.shape[0]
    width = x_ref.shape[1]
    owned = width // (ng * H)
    slots = 2 * ng
    chunks = H // 2
    span = 2 * length

    def mate(k):
        return (g * H + flip(r, k), core)

    loads = []
    for n, (src, dst) in enumerate(
        ((c_hbm, c_ref), (x_hbm, x_ref), (wq_hbm, wq_ref), (wk_hbm, wk_ref), (wv_hbm, wv_ref))
    ):
        copy = pltpu.make_async_copy(src, dst, load.at[n])
        copy.start()
        loads.append(copy)

    peers = [mate(k) for k in range(1, H)] + [(seq, other)]
    peers += [(g * H + flip(r, bit), other) for bit in BITS]
    for d in range(1, ng):
        far = (g + d) % ng
        peers.append((far * H + r, core))
    barrier = pltpu.get_barrier_semaphore()
    for peer in peers:
        pl.semaphore_signal(barrier, inc=1, device_id=peer, device_id_type=MESH)

    cut = 2 * DK + DV
    loads[0].wait()
    for h in range(H):
        own[h, cut:, :] = c_ref[:, h * DV : (h + 1) * DV].astype(F32).T
    pl.semaphore_wait(barrier, len(peers))
    ups = []
    for k in range(1, H):
        src = own.at[flip(r, k), pl.ds(cut, DV)]
        ups.append(push(src, rec.at[r, pl.ds(cut, DV)], us.at[k], ur.at[k], mate(k)))
    loads[1].wait()
    x = x_ref[...]
    for n, w_ref in enumerate((wq_ref, wk_ref)):
        loads[2 + n].wait()
        flat = dot(x, w_ref[...], (1, 0)).T
        for h in range(H):
            own[h, n * DK : (n + 1) * DK, :] = flat[h * DK : (h + 1) * DK]
    loads[4].wait()
    for h in range(H):
        own[h, 2 * DK : cut, :] = dot(x, wv_ref[:, h * DV : (h + 1) * DV], (1, 0)).T
    qkv = []
    for k in range(1, H):
        src = own.at[flip(r, k), pl.ds(0, cut)]
        qkv.append(push(src, rec.at[r, pl.ds(0, cut)], qs.at[k], qr.at[k], mate(k)))
    rec[r] = own[r]

    for cls in range(PLANE):
        for a in range(slots):
            at = ((a // 2) * H + cls + PLANE * (a % 2)) * owned
            st[cls, :, a * owned : (a + 1) * owned] = x_ref[:, at : at + owned].astype(F32)
    shares = []
    for k in range(1, PLANE):
        src = st.at[flip(r, k) % PLANE]
        shares.append(push(src, xg.at[r], xs.at[k], xr.at[k], mate(k)))
    xg[r] = st[r % PLANE]

    def swap(k):
        at = flip(r, k)
        return push(xg.at[at], xp.at[at], ps.at[k], pr.at[k], (seq, other))

    nears = [swap(0)]

    causal = lax.broadcasted_iota(jnp.int32, (span, span), 0) <= lax.broadcasted_iota(
        jnp.int32, (span, span), 1
    )
    ones = (lax.broadcasted_iota(jnp.int32, (AUX, span), 0) == 0).astype(F32)
    first = lax.broadcasted_iota(jnp.int32, (AUX, span), 0) == 0

    def part(c, start, count):
        rows = slice(start, start + count)
        return jnp.concatenate([rec[2 * c, rows, :], rec[2 * c + 1, rows, :]], 1)

    def relay(src, dst, send, recv, sign):
        for d in range(1, ng):
            to = g + sign * d

            @pl.when((to >= 0) & (to < ng))
            def _():
                push(src, dst.at[d], send.at[d], recv.at[d], (to * H + r, core))

    def settle(src, dst, send, recv, sign):
        for d in range(1, ng):
            to = g + sign * d

            @pl.when((to >= 0) & (to < ng))
            def _():
                pltpu.make_async_remote_copy(
                    src, dst.at[d], send.at[d], recv.at[d], (to * H + r, core), MESH
                ).wait_send()

    def collect(src, dst, send, recv, sign, total):
        total[...] = jnp.zeros(total.shape, F32)
        for d in range(1, ng):
            frm = g - sign * d

            @pl.when((frm >= 0) & (frm < ng))
            def _():
                pltpu.make_async_remote_copy(
                    src, dst.at[d], send.at[d], recv.at[d], (frm * H + r, core), MESH
                ).wait_recv()
                total[...] += dst[d]

    for copy in ups + qkv:
        copy.wait_recv()

    values = jnp.zeros((FEATS, DV), F32)
    norms = jnp.zeros((AUX, FEATS), F32)
    norm_at = []
    for c in range(chunks):
        fq = phi(part(c, 0, DK) * 0.5).astype(BF)
        fk = phi(part(c, DK, DK) * 0.5).astype(BF)
        va = jnp.concatenate([part(c, 2 * DK, DV), ones], 0).astype(BF)
        fqs[c] = fq
        fks[c] = fk
        vas[c] = va
        pv[c] = values
        norm_at.append(norms)
        values = values + dot(fk, va[:DV], (1, 1))
        norms = norms + dot(va[DV:], fk, (1, 1))
    ssend[...] = pack(values, norms)
    relay(ssend, srecv, ss, sr, 1)

    for c in range(chunks):
        fq, fk, va = fqs[c], fks[c], vas[c]
        attn = halves(jnp.where(causal, dot(fk, fq, (0, 0)), 0.0))
        ah[c] = attn[0]
        al[c] = attn[1]
        top = dot2r(va, attn, (1, 0))
        if c > 0:
            top = top + jnp.concatenate(
                [dot2(halves(pv[c]), fq, (0, 0)), dot2(halves(norm_at[c]), fq, (1, 0))], 0
            )
        tops[c] = top

    collect(ssend, srecv, ss, sr, 1, sin)
    in_values, in_norms = unpack(sin[...])
    in_pair, in_norm_pair = halves(in_values), halves(in_norms)
    back = jnp.zeros((FEATS, DV), F32)
    back_norm = jnp.zeros((AUX, FEATS), F32)
    back_norm_at = [None] * chunks
    for c in reversed(range(chunks)):
        fq = fqs[c]
        top = tops[c] + jnp.concatenate(
            [dot2(in_pair, fq, (0, 0)), dot2(in_norm_pair, fq, (1, 0))], 0
        )
        scale = 1.0 / top[DV : DV + 1]
        numer = part(c, cut, DV) * scale
        denom = -jnp.sum(numer * top[:DV], 0, keepdims=True) * scale
        gn = halves(jnp.concatenate([numer, jnp.where(first, denom, 0.0)], 0))
        nh[c] = gn[0]
        nl[c] = gn[1]
        rv[c] = back
        back_norm_at[c] = back_norm
        back = back + dot2r(fq, (gn[0][:DV], gn[1][:DV]), (1, 1))
        back_norm = back_norm + dot2((gn[0][DV:], gn[1][DV:]), fq, (1, 1))
    rsend[...] = pack(back, back_norm)
    relay(rsend, rrecv, rs, rr, -1)
    def store(c, start, rows):
        half = 0 if start < HALF else 1
        at = start - half * HALF
        for b in range(2):
            o[2 * c + b, half, at : at + rows.shape[0], :] = rows[:, b * length : (b + 1) * length]

    for c in range(chunks):
        fq, fk, va = fqs[c], fks[c], vas[c]
        attn = (ah[c], al[c])
        gn = (nh[c], nl[c])
        ga = halves(jnp.where(causal, dot2r(va, gn, (0, 0)), 0.0))
        held = halves(pv[c] + in_values)
        held_norm = halves(norm_at[c] + in_norms)
        gfq = dot2r(fk, ga, (1, 0))
        gfq = gfq + dot3(held, (gn[0][:DV], gn[1][:DV]), (1, 0))
        gfq = gfq + dot3(held_norm, (gn[0][DV:], gn[1][DV:]), (0, 0))
        store(c, 0, pull(part(c, 0, DK) * 0.5, gfq) * 0.5)
        gv = dot3((gn[0][:DV], gn[1][:DV]), attn, (1, 1))
        gfk = dot2r(fq, ga, (1, 1))
        if c < chunks - 1:
            after = halves(rv[c])
            gv = gv + dot2(after, fk, (0, 0))
            gfk = gfk + dot2(after, va[:DV], (1, 0))
            gfk = gfk + dot2(halves(back_norm_at[c]), va[DV:], (0, 0))
        gvs[c] = gv
        gfks[c] = gfk

    collect(rsend, rrecv, rs, rr, -1, rin)
    in_values, in_norms = unpack(rin[...])
    in_pair, in_norm_pair = halves(in_values), halves(in_norms)
    for c in range(chunks):
        fk, va = fks[c], vas[c]
        gv = gvs[c] + dot2(in_pair, fk, (0, 0))
        gfk = gfks[c] + dot2(in_pair, va[:DV], (1, 0)) + dot2(in_norm_pair, va[DV:], (0, 0))
        store(c, DK, gv[: DV // 2])
        store(c, HALF + DK, gv[DV // 2 :])
        store(c, HALF, pull(part(c, DK, DK) * 0.5, gfk) * 0.5)

    pending = shares + ups + qkv
    base = (r // PLANE) * PLANE
    here = pl.ds(base, PLANE)
    there = pl.ds(PLANE - base, PLANE)
    place = r % PLANE
    side = r // PLANE

    def across(i):
        rows = pl.ds(i * ROWS, ROWS)
        for half in range(2):
            pending.append(
                push(
                    o.at[there, half, rows], gj.at[i, 1, 0, core], zs.at[i, half],
                    gr.at[i, 1, 0, core], (g * H + mirror, half),
                )
            )

    def direct(i):
        rows = pl.ds(i * ROWS, ROWS)
        for k in (1, 2):
            for half in range(2):
                pending.append(
                    push(
                        o.at[here, half, rows], gj.at[i, 0, k, core], gs.at[i, 0, k, half],
                        gr.at[i, 0, k, core], (g * H + flip(r, k), half),
                    )
                )
        pending.append(
            push(
                o.at[here, other, rows], gj.at[i, 0, 0, core], gs.at[i, 0, 0, 0],
                gr.at[i, 0, 0, core], (seq, other),
            )
        )

    def landed(ref, sem):
        pltpu.make_async_copy(ref, ref, sem).wait()

    def arrive(i, m, k):
        if m == 0 or k == 0:
            if k < PLANE - 1:
                for b in range(2):
                    landed(gj.at[i, m, k, b], gr.at[i, m, k, b])
                return
        landed(gj.at[i, m, k], gr.at[i, m, k, 0])

    def mirrored(i):
        arrive(i, 1, 0)
        for k in (1, 2):
            pending.append(
                push(
                    gj.at[i, 1, 0], gj.at[i, 1, k], gs.at[i, 1, k, 0], gr.at[i, 1, k, 0], mate(k)
                )
            )

    def turn(i, m):
        return 1 + (i + m) % 2

    def forward(i, m):
        k = turn(i, m)
        arrive(i, m, k)
        pending.append(
            push(
                gj.at[i, m, k], gj.at[i, m, PLANE - 1], hs.at[i, m],
                gr.at[i, m, PLANE - 1, 0], mate(PLANE - 1 - k),
            )
        )

    def multiply(i, m):
        arrive(i, m, PLANE - 1 - turn(i, m))
        arrive(i, m, PLANE - 1)
        if m == 0:
            landed(gj.at[i, 0, 0, other], gr.at[i, 0, 0, other])
        pending.append(
            push(
                gj.at[i, m, :, other, place], rt.at[core, i, m], ts.at[i, m], tr.at[i, m],
                (seq, other),
            )
        )
        rt[core, i, m] = gj[i, m, :, core, place]
        rows = []
        for k in range(PLANE):
            rows.append(
                jnp.concatenate([gj[i, m, k, b, j] for b in range(2) for j in range(PLANE)], 1)
            )
        grads = jnp.concatenate(rows, 0).astype(BF)
        product = dot(grads, xb[...].reshape(2 * PLANE * length, slots * owned), (1, 0))
        for a in range(slots):
            ls[i, m, a % 2, a // 2] = product[:, a * owned : (a + 1) * owned]
        pending.append(
            push(
                ls.at[i, m, 1 - side], lr.at[i, 1 - m], bs.at[i, m], br.at[i, 1 - m], mate(PLANE)
            )
        )

    def combine(i, m):
        landed(lr.at[i, m], br.at[i, m])
        for a in range(ng):
            acc[i, m, a] = ls[i, m, side, a] + lr[i, m, a]
        for d in range(1, ng):
            to = (g + d) % ng
            pending.append(
                push(
                    acc.at[i, m, to], l2.at[i, m, d], cs.at[i, m, d], cr.at[i, m, d],
                    (to * H + r, core),
                )
            )

    swaps = []

    def settled(i):
        for m in range(2):
            total = acc[i, m, g]
            for d in range(1, ng):
                landed(l2.at[i, m, d], cr.at[i, m, d])
                total = total + l2[i, m, d]
            for k in range(PLANE):
                f2[core, i, flip(mirror if m else r, k)] = total[k * ROWS : (k + 1) * ROWS]
        swaps.append(push(f2.at[core, i], f2.at[core, i], ds.at[i], dr.at[i], (seq, other)))

    def spread(u):
        if u < PIECES:
            direct(u)
        else:
            mirrored(u - PIECES)

    def relayed(u):
        forward(u % PIECES, u // PIECES)

    def product_of(u):
        multiply(u % PIECES, u // PIECES)
        if u >= PIECES:
            combine(u - PIECES, 1)

    def joined(u):
        if u >= PIECES:
            combine(u - PIECES, 0)

    def done(u):
        if u >= PIECES:
            settled(u - PIECES)

    units = 2 * PIECES
    stages = list(zip((spread, relayed, product_of, joined, done), LAGS))

    def run(begin, end, only):
        for t in range(begin, end):
            for n, (stage, lag) in enumerate(stages):
                if n in only and 0 <= t - lag < units:
                    stage(t - lag)

    for i in range(PIECES):
        across(i)
        if i < LEAD:
            spread(i)
    for i in range(PIECES):
        gj[i, 0, 0, core] = o[here, core, i * ROWS : (i + 1) * ROWS, :]
    for k in range(1, PLANE):
        shares[k - 1].wait_recv()
        nears.append(swap(k))
    pending += nears
    relayed(0)
    for copy in nears:
        copy.wait_recv()
    for j in range(PLANE):
        xb[core, j * length : (j + 1) * length, :] = xg[base + j].astype(BF)
        xb[other, j * length : (j + 1) * length, :] = xp[base + j].astype(BF)
    every = range(5)
    stop = units + LAGS[2]
    first_turn = max(LEAD, LAGS[1] + 1)
    if LEAD < first_turn:
        run(LEAD, first_turn, (0,))
    run(LAGS[1] + 1, LEAD, every[1:])
    run(first_turn, stop, every)
    for i in range(PIECES):
        for m in range(2):
            landed(rt.at[other, i, m], tr.at[i, m])

    def back_rows(h, half):
        low = [((h // bit + r // bit) % 2) * bit for bit in (1, 2)]
        m = (h // PLANE + r // PLANE) % 2
        return jnp.concatenate([rt[half, i, m, low[0] + low[1]] for i in range(PIECES)], 0)

    whole = [[back_rows(h, half) for half in range(2)] for h in range(H)]
    blocks = [jnp.concatenate([whole[h][n][:DK] for h in range(H)], 0) for n in range(2)]
    for h in range(H):
        blocks.append(jnp.concatenate([whole[h][0][DK:], whole[h][1][DK:]], 0))
    for n, block in enumerate(blocks):
        jt[:, n * DV : (n + 1) * DV] = block.T.astype(BF)
    step = 512
    for at in range(0, width, step):
        rows = slice(at, at + step)
        total = dot(jt[:, :DV], wq_ref[rows, :], (1, 1))
        total = total + dot(jt[:, DV : 2 * DV], wk_ref[rows, :], (1, 1))
        total = total + dot(jt[:, 2 * DV :], wv_ref[rows, :], (1, 1))
        gi_ref[:, rows] = total.astype(BF)

    run(stop, units + LAGS[4], every)
    for copy in swaps:
        copy.wait_recv()
    whole = [
        [jnp.concatenate([f2[n, i, h] for i in range(PIECES)], 0) for n in range(2)]
        for h in range(H)
    ]
    final = [jnp.concatenate([whole[h][n][:DK] for h in range(H)], 0) for n in range(2)]
    for h in range(H):
        final.append(jnp.concatenate([whole[h][0][DK:], whole[h][1][DK:]], 0))
    keep = owned // 2
    for n, block in enumerate(final):
        fs[n] = block.T
        out_ref[n] = fs[n, pl.ds(pl.multiple_of(core * keep, keep), keep), :]
    pending += swaps
    for copy in pending:
        copy.wait_send()
    settle(ssend, srecv, ss, sr, 1)
    settle(rsend, rrecv, rs, rr, -1)


def fused(tokens, upstream, weights, ng):
    length, width = tokens.shape
    owned = width // (ng * H)
    slots = 2 * ng
    chunks, span = H // 2, 2 * length
    vm = lambda *shape: pltpu.VMEM(shape, F32)
    half = lambda *shape: pltpu.VMEM(shape, BF)
    state = (FEATS + 16, DV)
    scratch = [half(length, width), half(length, H * DV)]
    scratch += [pltpu.VMEM(w.shape, w.dtype) for w in weights]
    scratch += [
        vm(H, 2 * DK + 2 * DV, length), vm(H, 2 * DK + 2 * DV, length),
        vm(PLANE, length, slots * owned), vm(H, length, slots * owned),
        vm(H, length, slots * owned), half(2, PLANE * length, slots * owned),
        half(chunks, FEATS, span), half(chunks, FEATS, span), half(chunks, DV + AUX, span),
        half(chunks, span, span), half(chunks, span, span),
        half(chunks, DV + AUX, span), half(chunks, DV + AUX, span),
        vm(chunks, DV + AUX, span), vm(chunks, FEATS, DV), vm(chunks, FEATS, DV),
        vm(chunks, DV, span), vm(chunks, FEATS, span),
        vm(*state), vm(ng, *state), vm(*state), vm(*state), vm(ng, *state), vm(*state),
        vm(H, 2, HALF, length), vm(PIECES, 2, PLANE, 2, PLANE, ROWS, length),
        vm(PIECES, 2, 2, ng, PLANE * ROWS, owned), vm(PIECES, 2, ng, PLANE * ROWS, owned),
        vm(PIECES, 2, ng, PLANE * ROWS, owned), vm(PIECES, 2, ng, PLANE * ROWS, owned),
        vm(2, PIECES, 2, PLANE, ROWS, length), half(length, H * DV + 2 * DV),
        vm(2, PIECES, H, ROWS, owned), vm(2 + H, owned, DV),
        sems(5),
        sems(H), sems(H), sems(H), sems(H), sems(PLANE), sems(PLANE),
        sems(PLANE), sems(PLANE), sems(ng), sems(ng), sems(ng), sems(ng),
        sems(PIECES, 2), sems(PIECES, 2, PLANE, 2), sems(PIECES, 2, PLANE, 2), sems(PIECES, 2),
        sems(PIECES, 2), sems(PIECES, 2), sems(PIECES, 2), sems(PIECES, 2),
        sems(PIECES, 2, ng), sems(PIECES, 2, ng), sems(PIECES), sems(PIECES),
    ]
    return pl.pallas_call(
        functools.partial(fused_kernel, ng),
        out_shape=[
            jax.ShapeDtypeStruct((length, width), BF),
            jax.ShapeDtypeStruct((2 + H, owned // 2, DV), F32),
        ],
        in_specs=[HBM] * 5,
        out_specs=[VMEM] * 2,
        scratch_shapes=scratch,
        compiler_params=pltpu.CompilerParams(
            collective_id=0, has_side_effects=True, vmem_limit_bytes=60 << 20
        ),
    )(tokens, upstream, *weights)


def finish_kernel(gi_ref, o_ref, in_ref, oq_ref, ok_ref, ov_ref):
    in_ref[0] = gi_ref[...]
    oq_ref[...] = o_ref[0]
    ok_ref[...] = o_ref[1]
    for n in range(H):
        ov_ref[:, n * DV : (n + 1) * DV] = o_ref[2 + n]


def finish(grad_in, blocks):
    _, rows, lanes = blocks.shape
    return pl.pallas_call(
        finish_kernel,
        out_shape=[
            jax.ShapeDtypeStruct((1,) + grad_in.shape, BF),
            jax.ShapeDtypeStruct((rows, lanes), F32),
            jax.ShapeDtypeStruct((rows, lanes), F32),
            jax.ShapeDtypeStruct((rows, H * lanes), F32),
        ],
        in_specs=[VMEM] * 2,
        out_specs=[VMEM] * 4,
    )(grad_in, blocks)


def body(inputs, cotangent, w_query, w_key, w_value):
    ng = lax.axis_size("seq") // H
    weights = (w_query, w_key, w_value)
    return tuple(finish(*fused(inputs[0], cotangent[0], weights, ng)))


def solution(mesh):
    in_specs = (P("batch", "seq", None), P("batch", "seq", None), P(), P(), P())
    out_specs = (
        P("batch", "seq", None),
        P(("seq", "batch"), None),
        P(("seq", "batch"), None),
        P(("seq", "batch"), None),
    )
    return jax.shard_map(body, mesh=mesh, in_specs=in_specs, out_specs=out_specs, check_vma=False)
```

```python
import functools
import math

import jax
import jax.numpy as jnp
from jax import lax
from jax.experimental import pallas as pl
from jax.experimental.pallas import tpu as pltpu
from jax.sharding import PartitionSpec as P

H = 8
DK = 16
DV = 128
AUX = 16
PAIRS = DK * (DK + 1) // 2
FEATS = PAIRS + DK + 8
HALF = DK + DV // 2
PIECES = 5
ROWS = HALF // PIECES
BITS = (1, 2, 4)
PLANE = 4
LAGS = (0, 2, 4, 7, 10)
LEAD = 3
MESH = pl.DeviceIdType.MESH
BF = jnp.bfloat16
F32 = jnp.float32
VMEM = pl.BlockSpec(memory_space=pltpu.VMEM)
HBM = pl.BlockSpec(memory_space=pl.ANY)


def push(src, dst, send, recv, device):
    copy = pltpu.make_async_remote_copy(
        src_ref=src,
        dst_ref=dst,
        send_sem=send,
        recv_sem=recv,
        device_id=device,
        device_id_type=MESH,
    )
    copy.start()
    return copy


def sems(*sizes):
    return pltpu.SemaphoreType.DMA(sizes)


def dot(left, right, dims):
    return lax.dot_general(left, right, ((dims[:1], dims[1:]), ((), ())), preferred_element_type=F32)


def halves(a):
    high = a.astype(BF)
    return high, (a - high.astype(F32)).astype(BF)


def dot2(pair, right, dims):
    return dot(pair[0], right, dims) + dot(pair[1], right, dims)


def dot2r(left, pair, dims):
    return dot(left, pair[0], dims) + dot(left, pair[1], dims)


def dot3(lefts, rights, dims):
    return (
        dot(lefts[0], rights[0], dims)
        + dot(lefts[0], rights[1], dims)
        + dot(lefts[1], rights[0], dims)
    )


def flip(rank, mask):
    for bit in BITS:
        if mask & bit:
            rank = rank + bit - 2 * bit * ((rank // bit) % 2)
    return rank


def phi(u):
    half = DK // 2
    lanes = u.shape[1]
    pieces = [u * u * math.sqrt(0.5)]
    for s in range(1, half):
        pieces.append(u * pltpu.roll(u, DK - s, 0))
    pieces.append(u[:half] * u[half:])
    pieces.append(u)
    pieces.append((lax.broadcasted_iota(jnp.int32, (8, lanes), 0) == 0).astype(F32))
    return jnp.concatenate(pieces, 0)


def pull(u, grad):
    half = DK // 2
    total = grad[PAIRS : PAIRS + DK] + grad[:DK] * u * math.sqrt(2.0)
    for s in range(1, half):
        piece = grad[s * DK : (s + 1) * DK]
        total = total + piece * pltpu.roll(u, DK - s, 0) + pltpu.roll(piece * u, s, 0)
    last = grad[half * DK : half * DK + half]
    return total + jnp.concatenate([last * u[half:], last * u[:half]], 0)


def pack(values, norms):
    low = norms[:8, :DV]
    high = jnp.concatenate([norms[:8, DV:], jnp.zeros((8, 2 * DV - FEATS), F32)], 1)
    return jnp.concatenate([values, low, high], 0)


def unpack(packed):
    values = packed[:FEATS]
    norms = jnp.concatenate([packed[FEATS : FEATS + 8], packed[FEATS + 8 :, : FEATS - DV]], 1)
    return values, jnp.concatenate([norms, jnp.zeros((AUX - 8, FEATS), F32)], 0)


def fused_kernel(
    ng, x_hbm, c_hbm, wq_hbm, wk_hbm, wv_hbm, gi_hbm, out_ref,
    gi_ref, x_ref, c_ref, wq_ref, wk_ref, wv_ref, own, rec, st, xg, xp, xb,
    fqs, fks, vas, ah, al, nh, nl, tops, pv, rv, gvs, gfks,
    ssend, srecv, sin, rsend, rrecv, rin, o, gj, ls, lr, acc, l2, rt, jt, f2, fs,
    load, save, us, ur, qs, qr, xs, xr, ps, pr, ss, sr, rs, rr,
    zs, gs, gr, hs, ts, tr, bs, br, cs, cr, ds, dr,
):
    seq = lax.axis_index("seq")
    core = lax.axis_index("batch")
    other = 1 - core
    g = seq // H
    r = seq % H
    mirror = flip(r, PLANE)
    length = x_ref.shape[0]
    width = x_ref.shape[1]
    owned = width // (ng * H)
    slots = 2 * ng
    chunks = H // 2
    span = 2 * length

    def mate(k):
        return (g * H + flip(r, k), core)

    loads = []
    for n, (src, dst) in enumerate(
        ((c_hbm, c_ref), (x_hbm, x_ref), (wq_hbm, wq_ref), (wk_hbm, wk_ref), (wv_hbm, wv_ref))
    ):
        copy = pltpu.make_async_copy(src, dst, load.at[n])
        copy.start()
        loads.append(copy)

    peers = [mate(k) for k in range(1, H)] + [(seq, other)]
    peers += [(g * H + flip(r, bit), other) for bit in BITS]
    for d in range(1, ng):
        far = (g + d) % ng
        peers.append((far * H + r, core))
    barrier = pltpu.get_barrier_semaphore()
    for peer in peers:
        pl.semaphore_signal(barrier, inc=1, device_id=peer, device_id_type=MESH)

    cut = 2 * DK + DV
    loads[0].wait()
    for h in range(H):
        own[h, cut:, :] = c_ref[:, h * DV : (h + 1) * DV].astype(F32).T
    pl.semaphore_wait(barrier, len(peers))
    ups = []
    for k in range(1, H):
        src = own.at[flip(r, k), pl.ds(cut, DV)]
        ups.append(push(src, rec.at[r, pl.ds(cut, DV)], us.at[k], ur.at[k], mate(k)))
    loads[1].wait()
    x = x_ref[...]
    for n, w_ref in enumerate((wq_ref, wk_ref)):
        loads[2 + n].wait()
        flat = dot(x, w_ref[...], (1, 0)).T
        for h in range(H):
            own[h, n * DK : (n + 1) * DK, :] = flat[h * DK : (h + 1) * DK]
    loads[4].wait()
    for h in range(H):
        own[h, 2 * DK : cut, :] = dot(x, wv_ref[:, h * DV : (h + 1) * DV], (1, 0)).T
    qkv = []
    for k in range(1, H):
        src = own.at[flip(r, k), pl.ds(0, cut)]
        qkv.append(push(src, rec.at[r, pl.ds(0, cut)], qs.at[k], qr.at[k], mate(k)))
    rec[r] = own[r]

    for cls in range(PLANE):
        for a in range(slots):
            at = ((a // 2) * H + cls + PLANE * (a % 2)) * owned
            st[cls, :, a * owned : (a + 1) * owned] = x_ref[:, at : at + owned].astype(F32)
    shares = []
    for k in range(1, PLANE):
        src = st.at[flip(r, k) % PLANE]
        shares.append(push(src, xg.at[r], xs.at[k], xr.at[k], mate(k)))
    xg[r] = st[r % PLANE]

    def swap(k):
        at = flip(r, k)
        return push(xg.at[at], xp.at[at], ps.at[k], pr.at[k], (seq, other))

    nears = [swap(0)]

    causal = lax.broadcasted_iota(jnp.int32, (span, span), 0) <= lax.broadcasted_iota(
        jnp.int32, (span, span), 1
    )
    ones = (lax.broadcasted_iota(jnp.int32, (AUX, span), 0) == 0).astype(F32)
    first = lax.broadcasted_iota(jnp.int32, (AUX, span), 0) == 0

    def part(c, start, count):
        rows = slice(start, start + count)
        return jnp.concatenate([rec[2 * c, rows, :], rec[2 * c + 1, rows, :]], 1)

    def relay(src, dst, send, recv, sign):
        for d in range(1, ng):
            to = g + sign * d

            @pl.when((to >= 0) & (to < ng))
            def _():
                push(src, dst.at[d], send.at[d], recv.at[d], (to * H + r, core))

    def settle(src, dst, send, recv, sign):
        for d in range(1, ng):
            to = g + sign * d

            @pl.when((to >= 0) & (to < ng))
            def _():
                pltpu.make_async_remote_copy(
                    src, dst.at[d], send.at[d], recv.at[d], (to * H + r, core), MESH
                ).wait_send()

    def collect(src, dst, send, recv, sign, total):
        total[...] = jnp.zeros(total.shape, F32)
        for d in range(1, ng):
            frm = g - sign * d

            @pl.when((frm >= 0) & (frm < ng))
            def _():
                pltpu.make_async_remote_copy(
                    src, dst.at[d], send.at[d], recv.at[d], (frm * H + r, core), MESH
                ).wait_recv()
                total[...] += dst[d]

    for copy in ups + qkv:
        copy.wait_recv()

    values = jnp.zeros((FEATS, DV), F32)
    norms = jnp.zeros((AUX, FEATS), F32)
    norm_at = []
    for c in range(chunks):
        fq = phi(part(c, 0, DK) * 0.5).astype(BF)
        fk = phi(part(c, DK, DK) * 0.5).astype(BF)
        va = jnp.concatenate([part(c, 2 * DK, DV), ones], 0).astype(BF)
        fqs[c] = fq
        fks[c] = fk
        vas[c] = va
        pv[c] = values
        norm_at.append(norms)
        values = values + dot(fk, va[:DV], (1, 1))
        norms = norms + dot(va[DV:], fk, (1, 1))
    ssend[...] = pack(values, norms)
    relay(ssend, srecv, ss, sr, 1)

    for c in range(chunks):
        fq, fk, va = fqs[c], fks[c], vas[c]
        attn = halves(jnp.where(causal, dot(fk, fq, (0, 0)), 0.0))
        ah[c] = attn[0]
        al[c] = attn[1]
        top = dot2r(va, attn, (1, 0))
        if c > 0:
            top = top + jnp.concatenate(
                [dot2(halves(pv[c]), fq, (0, 0)), dot2(halves(norm_at[c]), fq, (1, 0))], 0
            )
        tops[c] = top

    collect(ssend, srecv, ss, sr, 1, sin)
    in_values, in_norms = unpack(sin[...])
    in_pair, in_norm_pair = halves(in_values), halves(in_norms)
    back = jnp.zeros((FEATS, DV), F32)
    back_norm = jnp.zeros((AUX, FEATS), F32)
    back_norm_at = [None] * chunks
    for c in reversed(range(chunks)):
        fq = fqs[c]
        top = tops[c] + jnp.concatenate(
            [dot2(in_pair, fq, (0, 0)), dot2(in_norm_pair, fq, (1, 0))], 0
        )
        scale = 1.0 / top[DV : DV + 1]
        numer = part(c, cut, DV) * scale
        denom = -jnp.sum(numer * top[:DV], 0, keepdims=True) * scale
        gn = halves(jnp.concatenate([numer, jnp.where(first, denom, 0.0)], 0))
        nh[c] = gn[0]
        nl[c] = gn[1]
        rv[c] = back
        back_norm_at[c] = back_norm
        back = back + dot2r(fq, (gn[0][:DV], gn[1][:DV]), (1, 1))
        back_norm = back_norm + dot2((gn[0][DV:], gn[1][DV:]), fq, (1, 1))
    rsend[...] = pack(back, back_norm)
    relay(rsend, rrecv, rs, rr, -1)
    def store(c, start, rows):
        half = 0 if start < HALF else 1
        at = start - half * HALF
        for b in range(2):
            o[2 * c + b, half, at : at + rows.shape[0], :] = rows[:, b * length : (b + 1) * length]

    for c in range(chunks):
        fq, fk, va = fqs[c], fks[c], vas[c]
        attn = (ah[c], al[c])
        gn = (nh[c], nl[c])
        ga = halves(jnp.where(causal, dot2r(va, gn, (0, 0)), 0.0))
        held = halves(pv[c] + in_values)
        held_norm = halves(norm_at[c] + in_norms)
        gfq = dot2r(fk, ga, (1, 0))
        gfq = gfq + dot3(held, (gn[0][:DV], gn[1][:DV]), (1, 0))
        gfq = gfq + dot3(held_norm, (gn[0][DV:], gn[1][DV:]), (0, 0))
        store(c, 0, pull(part(c, 0, DK) * 0.5, gfq) * 0.5)
        gv = dot3((gn[0][:DV], gn[1][:DV]), attn, (1, 1))
        gfk = dot2r(fq, ga, (1, 1))
        if c < chunks - 1:
            after = halves(rv[c])
            gv = gv + dot2(after, fk, (0, 0))
            gfk = gfk + dot2(after, va[:DV], (1, 0))
            gfk = gfk + dot2(halves(back_norm_at[c]), va[DV:], (0, 0))
        gvs[c] = gv
        gfks[c] = gfk

    collect(rsend, rrecv, rs, rr, -1, rin)
    in_values, in_norms = unpack(rin[...])
    in_pair, in_norm_pair = halves(in_values), halves(in_norms)
    for c in range(chunks):
        fk, va = fks[c], vas[c]
        gv = gvs[c] + dot2(in_pair, fk, (0, 0))
        gfk = gfks[c] + dot2(in_pair, va[:DV], (1, 0)) + dot2(in_norm_pair, va[DV:], (0, 0))
        store(c, DK, gv[: DV // 2])
        store(c, HALF + DK, gv[DV // 2 :])
        store(c, HALF, pull(part(c, DK, DK) * 0.5, gfk) * 0.5)

    pending = shares + ups + qkv
    base = (r // PLANE) * PLANE
    here = pl.ds(base, PLANE)
    there = pl.ds(PLANE - base, PLANE)
    place = r % PLANE
    side = r // PLANE

    def across(i):
        rows = pl.ds(i * ROWS, ROWS)
        for half in range(2):
            pending.append(
                push(
                    o.at[there, half, rows], gj.at[i, 1, 0, core], zs.at[i, half],
                    gr.at[i, 1, 0, core], (g * H + mirror, half),
                )
            )

    def direct(i):
        rows = pl.ds(i * ROWS, ROWS)
        for k in (1, 2):
            for half in range(2):
                pending.append(
                    push(
                        o.at[here, half, rows], gj.at[i, 0, k, core], gs.at[i, 0, k, half],
                        gr.at[i, 0, k, core], (g * H + flip(r, k), half),
                    )
                )
        pending.append(
            push(
                o.at[here, other, rows], gj.at[i, 0, 0, core], gs.at[i, 0, 0, 0],
                gr.at[i, 0, 0, core], (seq, other),
            )
        )

    def landed(ref, sem):
        pltpu.make_async_copy(ref, ref, sem).wait()

    def arrive(i, m, k):
        if m == 0 or k == 0:
            if k < PLANE - 1:
                for b in range(2):
                    landed(gj.at[i, m, k, b], gr.at[i, m, k, b])
                return
        landed(gj.at[i, m, k], gr.at[i, m, k, 0])

    def mirrored(i):
        arrive(i, 1, 0)
        for k in (1, 2):
            pending.append(
                push(
                    gj.at[i, 1, 0], gj.at[i, 1, k], gs.at[i, 1, k, 0], gr.at[i, 1, k, 0], mate(k)
                )
            )

    def turn(i, m):
        return 1 + (i + m) % 2

    def forward(i, m):
        k = turn(i, m)
        arrive(i, m, k)
        pending.append(
            push(
                gj.at[i, m, k], gj.at[i, m, PLANE - 1], hs.at[i, m],
                gr.at[i, m, PLANE - 1, 0], mate(PLANE - 1 - k),
            )
        )

    def multiply(i, m):
        arrive(i, m, PLANE - 1 - turn(i, m))
        arrive(i, m, PLANE - 1)
        if m == 0:
            landed(gj.at[i, 0, 0, other], gr.at[i, 0, 0, other])
        pending.append(
            push(
                gj.at[i, m, :, other, place], rt.at[core, i, m], ts.at[i, m], tr.at[i, m],
                (seq, other),
            )
        )
        rt[core, i, m] = gj[i, m, :, core, place]
        rows = []
        for k in range(PLANE):
            rows.append(
                jnp.concatenate([gj[i, m, k, b, j] for b in range(2) for j in range(PLANE)], 1)
            )
        grads = jnp.concatenate(rows, 0).astype(BF)
        product = dot(grads, xb[...].reshape(2 * PLANE * length, slots * owned), (1, 0))
        for a in range(slots):
            ls[i, m, a % 2, a // 2] = product[:, a * owned : (a + 1) * owned]
        pending.append(
            push(
                ls.at[i, m, 1 - side], lr.at[i, 1 - m], bs.at[i, m], br.at[i, 1 - m], mate(PLANE)
            )
        )

    def combine(i, m):
        landed(lr.at[i, m], br.at[i, m])
        for a in range(ng):
            acc[i, m, a] = ls[i, m, side, a] + lr[i, m, a]
        for d in range(1, ng):
            to = (g + d) % ng
            pending.append(
                push(
                    acc.at[i, m, to], l2.at[i, m, d], cs.at[i, m, d], cr.at[i, m, d],
                    (to * H + r, core),
                )
            )

    swaps = []

    def settled(i):
        for m in range(2):
            total = acc[i, m, g]
            for d in range(1, ng):
                landed(l2.at[i, m, d], cr.at[i, m, d])
                total = total + l2[i, m, d]
            for k in range(PLANE):
                f2[core, i, flip(mirror if m else r, k)] = total[k * ROWS : (k + 1) * ROWS]
        swaps.append(push(f2.at[core, i], f2.at[core, i], ds.at[i], dr.at[i], (seq, other)))

    order = [(0, 0)]
    for i in range(1, PIECES):
        order += [(i, 0), (i - 1, 1)]
    order.append((PIECES - 1, 1))

    def spread(u):
        i, m = order[u]
        if m == 0:
            direct(i)
        else:
            mirrored(i)

    def relayed(u):
        forward(*order[u])

    def product_of(u):
        i, m = order[u]
        multiply(i, m)
        if m == 1:
            combine(i, 1)

    def joined(u):
        i, m = order[u]
        if m == 1:
            combine(i, 0)

    def done(u):
        i, m = order[u]
        if m == 1:
            settled(i)

    units = 2 * PIECES
    stages = list(zip((spread, relayed, product_of, joined, done), LAGS))

    def run(begin, end, only):
        for t in range(begin, end):
            for n, (stage, lag) in enumerate(stages):
                if n in only and 0 <= t - lag < units:
                    stage(t - lag)

    for i in range(PIECES):
        across(i)
        if i < LEAD:
            spread(i)
    for i in range(PIECES):
        gj[i, 0, 0, core] = o[here, core, i * ROWS : (i + 1) * ROWS, :]
    for k in range(1, PLANE):
        shares[k - 1].wait_recv()
        nears.append(swap(k))
    pending += nears
    relayed(0)
    for copy in nears:
        copy.wait_recv()
    for j in range(PLANE):
        xb[core, j * length : (j + 1) * length, :] = xg[base + j].astype(BF)
        xb[other, j * length : (j + 1) * length, :] = xp[base + j].astype(BF)
    every = range(5)
    stop = units + LAGS[2]
    first_turn = max(LEAD, LAGS[1] + 1)
    if LEAD < first_turn:
        run(LEAD, first_turn, (0,))
    run(LAGS[1] + 1, LEAD, every[1:])
    run(first_turn, stop, every)
    for u in range(stop - LAGS[3], units - 1):
        joined(u)
    for i in range(PIECES):
        for m in range(2):
            landed(rt.at[other, i, m], tr.at[i, m])

    def back_rows(h, half):
        low = [((h // bit + r // bit) % 2) * bit for bit in (1, 2)]
        m = (h // PLANE + r // PLANE) % 2
        return jnp.concatenate([rt[half, i, m, low[0] + low[1]] for i in range(PIECES)], 0)

    whole = [[back_rows(h, half) for half in range(2)] for h in range(H)]
    blocks = [jnp.concatenate([whole[h][n][:DK] for h in range(H)], 0) for n in range(2)]
    for h in range(H):
        blocks.append(jnp.concatenate([whole[h][0][DK:], whole[h][1][DK:]], 0))
    for n, block in enumerate(blocks):
        jt[:, n * DV : (n + 1) * DV] = block.T.astype(BF)
    stores = []

    def flow(begin, end, step):
        for at in range(begin, end, step):
            rows = slice(at, at + step)
            total = dot(jt[:, :DV], wq_ref[rows, :], (1, 1))
            total = total + dot(jt[:, DV : 2 * DV], wk_ref[rows, :], (1, 1))
            total = total + dot(jt[:, 2 * DV :], wv_ref[rows, :], (1, 1))
            gi_ref[:, rows] = total.astype(BF)
            copy = pltpu.make_async_copy(
                gi_ref.at[:, rows], gi_hbm.at[:, rows], save.at[at // step]
            )
            copy.start()
            stores.append(copy)

    flow(0, width // 2, width // 4)
    joined(units - 1)
    flow(width // 2, width, width // 4)

    for u in range(stop - LAGS[4], units):
        done(u)
    for copy in swaps:
        copy.wait_recv()
    whole = [
        [jnp.concatenate([f2[n, i, h] for i in range(PIECES)], 0) for n in range(2)]
        for h in range(H)
    ]
    final = [jnp.concatenate([whole[h][n][:DK] for h in range(H)], 0) for n in range(2)]
    for h in range(H):
        final.append(jnp.concatenate([whole[h][0][DK:], whole[h][1][DK:]], 0))
    keep = owned // 2
    for n, block in enumerate(final):
        fs[n] = block.T
        out_ref[n] = fs[n, pl.ds(pl.multiple_of(core * keep, keep), keep), :]
    pending += swaps
    for copy in pending:
        copy.wait_send()
    for copy in stores:
        copy.wait()
    settle(ssend, srecv, ss, sr, 1)
    settle(rsend, rrecv, rs, rr, -1)


def fused(tokens, upstream, weights, ng):
    length, width = tokens.shape
    owned = width // (ng * H)
    slots = 2 * ng
    chunks, span = H // 2, 2 * length
    vm = lambda *shape: pltpu.VMEM(shape, F32)
    half = lambda *shape: pltpu.VMEM(shape, BF)
    state = (FEATS + 16, DV)
    scratch = [half(length, width), half(length, width), half(length, H * DV)]
    scratch += [pltpu.VMEM(w.shape, w.dtype) for w in weights]
    scratch += [
        vm(H, 2 * DK + 2 * DV, length), vm(H, 2 * DK + 2 * DV, length),
        vm(PLANE, length, slots * owned), vm(H, length, slots * owned),
        vm(H, length, slots * owned), half(2, PLANE * length, slots * owned),
        half(chunks, FEATS, span), half(chunks, FEATS, span), half(chunks, DV + AUX, span),
        half(chunks, span, span), half(chunks, span, span),
        half(chunks, DV + AUX, span), half(chunks, DV + AUX, span),
        vm(chunks, DV + AUX, span), vm(chunks, FEATS, DV), vm(chunks, FEATS, DV),
        vm(chunks, DV, span), vm(chunks, FEATS, span),
        vm(*state), vm(ng, *state), vm(*state), vm(*state), vm(ng, *state), vm(*state),
        vm(H, 2, HALF, length), vm(PIECES, 2, PLANE, 2, PLANE, ROWS, length),
        vm(PIECES, 2, 2, ng, PLANE * ROWS, owned), vm(PIECES, 2, ng, PLANE * ROWS, owned),
        vm(PIECES, 2, ng, PLANE * ROWS, owned), vm(PIECES, 2, ng, PLANE * ROWS, owned),
        vm(2, PIECES, 2, PLANE, ROWS, length), half(length, H * DV + 2 * DV),
        vm(2, PIECES, H, ROWS, owned), vm(2 + H, owned, DV),
        sems(5), sems(4),
        sems(H), sems(H), sems(H), sems(H), sems(PLANE), sems(PLANE),
        sems(PLANE), sems(PLANE), sems(ng), sems(ng), sems(ng), sems(ng),
        sems(PIECES, 2), sems(PIECES, 2, PLANE, 2), sems(PIECES, 2, PLANE, 2), sems(PIECES, 2),
        sems(PIECES, 2), sems(PIECES, 2), sems(PIECES, 2), sems(PIECES, 2),
        sems(PIECES, 2, ng), sems(PIECES, 2, ng), sems(PIECES), sems(PIECES),
    ]
    return pl.pallas_call(
        functools.partial(fused_kernel, ng),
        out_shape=[
            jax.ShapeDtypeStruct((length, width), BF),
            jax.ShapeDtypeStruct((2 + H, owned // 2, DV), F32),
        ],
        in_specs=[HBM] * 5,
        out_specs=[HBM, VMEM],
        scratch_shapes=scratch,
        compiler_params=pltpu.CompilerParams(
            collective_id=0, has_side_effects=True, vmem_limit_bytes=60 << 20
        ),
    )(tokens, upstream, *weights)


def finish_kernel(gi_ref, o_ref, in_ref, oq_ref, ok_ref, ov_ref, grad, held, into, out):
    parts = into.shape[0] - 1
    rows = gi_ref.shape[0] // parts
    loads = [pltpu.make_async_copy(o_ref, held, into.at[parts])]
    for n in range(parts):
        at = pl.ds(n * rows, rows)
        loads.append(pltpu.make_async_copy(gi_ref.at[at], grad.at[at], into.at[n]))
    for copy in loads:
        copy.start()
    loads[0].wait()
    stores = [
        pltpu.make_async_copy(held.at[0], oq_ref, out.at[0]),
        pltpu.make_async_copy(held.at[1], ok_ref, out.at[1]),
    ]
    for n in range(H):
        columns = pl.ds(n * DV, DV)
        stores.append(
            pltpu.make_async_copy(held.at[2 + n], ov_ref.at[:, columns], out.at[2 + n])
        )
    for copy in stores:
        copy.start()
    for n in range(parts):
        at = pl.ds(n * rows, rows)
        loads[1 + n].wait()
        copy = pltpu.make_async_copy(grad.at[at], in_ref.at[0, at], out.at[2 + H + n])
        copy.start()
        stores.append(copy)
    for copy in stores:
        copy.wait()


def finish(grad_in, blocks):
    _, rows, lanes = blocks.shape
    parts = 4
    return pl.pallas_call(
        finish_kernel,
        out_shape=[
            jax.ShapeDtypeStruct((1,) + grad_in.shape, BF),
            jax.ShapeDtypeStruct((rows, lanes), F32),
            jax.ShapeDtypeStruct((rows, lanes), F32),
            jax.ShapeDtypeStruct((rows, H * lanes), F32),
        ],
        in_specs=[HBM] * 2,
        out_specs=[HBM] * 4,
        scratch_shapes=[
            pltpu.VMEM(grad_in.shape, BF),
            pltpu.VMEM(blocks.shape, F32),
            sems(1 + parts),
            sems(2 + H + parts),
        ],
    )(grad_in, blocks)


def body(inputs, cotangent, w_query, w_key, w_value):
    ng = lax.axis_size("seq") // H
    weights = (w_query, w_key, w_value)
    return tuple(finish(*fused(inputs[0], cotangent[0], weights, ng)))


def solution(mesh):
    in_specs = (P("batch", "seq", None), P("batch", "seq", None), P(), P(), P())
    out_specs = (
        P("batch", "seq", None),
        P(("seq", "batch"), None),
        P(("seq", "batch"), None),
        P(("seq", "batch"), None),
    )
    return jax.shard_map(body, mesh=mesh, in_specs=in_specs, out_specs=out_specs, check_vma=False)
```

```python
import functools
import math

import jax
import jax.numpy as jnp
from jax import lax
from jax.experimental import pallas as pl
from jax.experimental.pallas import tpu as pltpu
from jax.sharding import PartitionSpec as P

H = 8
DK = 16
DV = 128
AUX = 16
PAIRS = DK * (DK + 1) // 2
FEATS = PAIRS + DK + 8
HALF = DK + DV // 2
PIECES = 5
ROWS = HALF // PIECES
BITS = (1, 2, 4)
PLANE = 4
LAGS = (0, 2, 4, 7, 10)
LEAD = 3
MESH = pl.DeviceIdType.MESH
BF = jnp.bfloat16
F32 = jnp.float32
VMEM = pl.BlockSpec(memory_space=pltpu.VMEM)
HBM = pl.BlockSpec(memory_space=pl.ANY)


def push(src, dst, send, recv, device):
    copy = pltpu.make_async_remote_copy(
        src_ref=src,
        dst_ref=dst,
        send_sem=send,
        recv_sem=recv,
        device_id=device,
        device_id_type=MESH,
    )
    copy.start()
    return copy


def sems(*sizes):
    return pltpu.SemaphoreType.DMA(sizes)


def dot(left, right, dims):
    return lax.dot_general(left, right, ((dims[:1], dims[1:]), ((), ())), preferred_element_type=F32)


def halves(a):
    high = a.astype(BF)
    return high, (a - high.astype(F32)).astype(BF)


def dot2(pair, right, dims):
    return dot(pair[0], right, dims) + dot(pair[1], right, dims)


def dot2r(left, pair, dims):
    return dot(left, pair[0], dims) + dot(left, pair[1], dims)


def dot3(lefts, rights, dims):
    return (
        dot(lefts[0], rights[0], dims)
        + dot(lefts[0], rights[1], dims)
        + dot(lefts[1], rights[0], dims)
    )


def flip(rank, mask):
    for bit in BITS:
        if mask & bit:
            rank = rank + bit - 2 * bit * ((rank // bit) % 2)
    return rank


def phi(u):
    half = DK // 2
    lanes = u.shape[1]
    pieces = [u * u * math.sqrt(0.5)]
    for s in range(1, half):
        pieces.append(u * pltpu.roll(u, DK - s, 0))
    pieces.append(u[:half] * u[half:])
    pieces.append(u)
    pieces.append((lax.broadcasted_iota(jnp.int32, (8, lanes), 0) == 0).astype(F32))
    return jnp.concatenate(pieces, 0)


def pull(u, grad):
    half = DK // 2
    total = grad[PAIRS : PAIRS + DK] + grad[:DK] * u * math.sqrt(2.0)
    for s in range(1, half):
        piece = grad[s * DK : (s + 1) * DK]
        total = total + piece * pltpu.roll(u, DK - s, 0) + pltpu.roll(piece * u, s, 0)
    last = grad[half * DK : half * DK + half]
    return total + jnp.concatenate([last * u[half:], last * u[:half]], 0)


def pack(values, norms):
    low = norms[:8, :DV]
    high = jnp.concatenate([norms[:8, DV:], jnp.zeros((8, 2 * DV - FEATS), F32)], 1)
    return jnp.concatenate([values, low, high], 0)


def unpack(packed):
    values = packed[:FEATS]
    norms = jnp.concatenate([packed[FEATS : FEATS + 8], packed[FEATS + 8 :, : FEATS - DV]], 1)
    return values, jnp.concatenate([norms, jnp.zeros((AUX - 8, FEATS), F32)], 0)


def fused_kernel(
    ng, x_hbm, c_hbm, wq_hbm, wk_hbm, wv_hbm, gi_hbm, out_ref,
    gi_ref, x_ref, c_ref, wq_ref, wk_ref, wv_ref, own, rec, st, xg, xp, xb,
    fqs, fks, vas, ah, al, nh, nl, tops, pv, rv, gvs, gfks,
    ssend, srecv, sin, rsend, rrecv, rin, o, gj, ls, lr, acc, l2, rt, jt, f2, fs,
    load, save, us, ur, qs, qr, xs, xr, ps, pr, ss, sr, rs, rr,
    zs, gs, gr, hs, ts, tr, bs, br, cs, cr, ds, dr,
):
    seq = lax.axis_index("seq")
    core = lax.axis_index("batch")
    other = 1 - core
    g = seq // H
    r = seq % H
    mirror = flip(r, PLANE)
    length = x_ref.shape[0]
    width = x_ref.shape[1]
    owned = width // (ng * H)
    slots = 2 * ng
    chunks = H // 2
    span = 2 * length

    def mate(k):
        return (g * H + flip(r, k), core)

    loads = []
    for n, (src, dst) in enumerate(
        ((c_hbm, c_ref), (x_hbm, x_ref), (wq_hbm, wq_ref), (wk_hbm, wk_ref), (wv_hbm, wv_ref))
    ):
        copy = pltpu.make_async_copy(src, dst, load.at[n])
        copy.start()
        loads.append(copy)

    peers = [mate(k) for k in range(1, H)] + [(seq, other)]
    peers += [(g * H + flip(r, bit), other) for bit in BITS]
    for d in range(1, ng):
        far = (g + d) % ng
        peers.append((far * H + r, core))
    barrier = pltpu.get_barrier_semaphore()
    for peer in peers:
        pl.semaphore_signal(barrier, inc=1, device_id=peer, device_id_type=MESH)

    cut = 2 * DK + DV
    loads[0].wait()
    for h in range(H):
        own[h, cut:, :] = c_ref[:, h * DV : (h + 1) * DV].astype(F32).T
    pl.semaphore_wait(barrier, len(peers))
    ups = []
    for k in range(1, H):
        src = own.at[flip(r, k), pl.ds(cut, DV)]
        ups.append(push(src, rec.at[r, pl.ds(cut, DV)], us.at[k], ur.at[k], mate(k)))
    loads[1].wait()
    x = x_ref[...]
    for n, w_ref in enumerate((wq_ref, wk_ref)):
        loads[2 + n].wait()
        flat = dot(x, w_ref[...], (1, 0)).T
        for h in range(H):
            own[h, n * DK : (n + 1) * DK, :] = flat[h * DK : (h + 1) * DK]
    loads[4].wait()
    for h in range(H):
        own[h, 2 * DK : cut, :] = dot(x, wv_ref[:, h * DV : (h + 1) * DV], (1, 0)).T
    qkv = []
    for k in range(1, H):
        src = own.at[flip(r, k), pl.ds(0, cut)]
        qkv.append(push(src, rec.at[r, pl.ds(0, cut)], qs.at[k], qr.at[k], mate(k)))
    rec[r] = own[r]

    for cls in range(PLANE):
        for a in range(slots):
            at = ((a // 2) * H + cls + PLANE * (a % 2)) * owned
            st[cls, :, a * owned : (a + 1) * owned] = x_ref[:, at : at + owned].astype(F32)
    shares = []
    for k in range(1, PLANE):
        src = st.at[flip(r, k) % PLANE]
        shares.append(push(src, xg.at[r], xs.at[k], xr.at[k], mate(k)))
    xg[r] = st[r % PLANE]

    def swap(k):
        at = flip(r, k)
        return push(xg.at[at], xp.at[at], ps.at[k], pr.at[k], (seq, other))

    nears = [swap(0)]

    causal = lax.broadcasted_iota(jnp.int32, (span, span), 0) <= lax.broadcasted_iota(
        jnp.int32, (span, span), 1
    )
    ones = (lax.broadcasted_iota(jnp.int32, (AUX, span), 0) == 0).astype(F32)
    first = lax.broadcasted_iota(jnp.int32, (AUX, span), 0) == 0

    def part(c, start, count):
        rows = slice(start, start + count)
        return jnp.concatenate([rec[2 * c, rows, :], rec[2 * c + 1, rows, :]], 1)

    def relay(src, dst, send, recv, sign):
        for d in range(1, ng):
            to = g + sign * d

            @pl.when((to >= 0) & (to < ng))
            def _():
                push(src, dst.at[d], send.at[d], recv.at[d], (to * H + r, core))

    def settle(src, dst, send, recv, sign):
        for d in range(1, ng):
            to = g + sign * d

            @pl.when((to >= 0) & (to < ng))
            def _():
                pltpu.make_async_remote_copy(
                    src, dst.at[d], send.at[d], recv.at[d], (to * H + r, core), MESH
                ).wait_send()

    def collect(src, dst, send, recv, sign, total):
        total[...] = jnp.zeros(total.shape, F32)
        for d in range(1, ng):
            frm = g - sign * d

            @pl.when((frm >= 0) & (frm < ng))
            def _():
                pltpu.make_async_remote_copy(
                    src, dst.at[d], send.at[d], recv.at[d], (frm * H + r, core), MESH
                ).wait_recv()
                total[...] += dst[d]

    for copy in qkv:
        copy.wait_recv()

    values = jnp.zeros((FEATS, DV), F32)
    norms = jnp.zeros((AUX, FEATS), F32)
    norm_at = []
    for c in range(chunks):
        fk = phi(part(c, DK, DK) * 0.5).astype(BF)
        va = jnp.concatenate([part(c, 2 * DK, DV), ones], 0).astype(BF)
        fks[c] = fk
        vas[c] = va
        pv[c] = values
        norm_at.append(norms)
        values = values + dot(fk, va[:DV], (1, 1))
        norms = norms + dot(va[DV:], fk, (1, 1))
    ssend[...] = pack(values, norms)
    relay(ssend, srecv, ss, sr, 1)

    for c in range(chunks):
        fq = phi(part(c, 0, DK) * 0.5).astype(BF)
        fqs[c] = fq
        fk, va = fks[c], vas[c]
        attn = halves(jnp.where(causal, dot(fk, fq, (0, 0)), 0.0))
        ah[c] = attn[0]
        al[c] = attn[1]
        top = dot2r(va, attn, (1, 0))
        if c > 0:
            top = top + jnp.concatenate(
                [dot2(halves(pv[c]), fq, (0, 0)), dot2(halves(norm_at[c]), fq, (1, 0))], 0
            )
        tops[c] = top

    collect(ssend, srecv, ss, sr, 1, sin)
    for copy in ups:
        copy.wait_recv()
    in_values, in_norms = unpack(sin[...])
    in_pair, in_norm_pair = halves(in_values), halves(in_norms)
    back = jnp.zeros((FEATS, DV), F32)
    back_norm = jnp.zeros((AUX, FEATS), F32)
    back_norm_at = [None] * chunks
    for c in reversed(range(chunks)):
        fq = fqs[c]
        top = tops[c] + jnp.concatenate(
            [dot2(in_pair, fq, (0, 0)), dot2(in_norm_pair, fq, (1, 0))], 0
        )
        scale = 1.0 / top[DV : DV + 1]
        numer = part(c, cut, DV) * scale
        denom = -jnp.sum(numer * top[:DV], 0, keepdims=True) * scale
        gn = halves(jnp.concatenate([numer, jnp.where(first, denom, 0.0)], 0))
        nh[c] = gn[0]
        nl[c] = gn[1]
        rv[c] = back
        back_norm_at[c] = back_norm
        back = back + dot2r(fq, (gn[0][:DV], gn[1][:DV]), (1, 1))
        back_norm = back_norm + dot2((gn[0][DV:], gn[1][DV:]), fq, (1, 1))
    rsend[...] = pack(back, back_norm)
    relay(rsend, rrecv, rs, rr, -1)
    def store(c, start, rows):
        half = 0 if start < HALF else 1
        at = start - half * HALF
        for b in range(2):
            o[2 * c + b, half, at : at + rows.shape[0], :] = rows[:, b * length : (b + 1) * length]

    for c in range(chunks):
        fq, fk, va = fqs[c], fks[c], vas[c]
        attn = (ah[c], al[c])
        gn = (nh[c], nl[c])
        ga = halves(jnp.where(causal, dot2r(va, gn, (0, 0)), 0.0))
        held = halves(pv[c] + in_values)
        held_norm = halves(norm_at[c] + in_norms)
        gfq = dot2r(fk, ga, (1, 0))
        gfq = gfq + dot3(held, (gn[0][:DV], gn[1][:DV]), (1, 0))
        gfq = gfq + dot3(held_norm, (gn[0][DV:], gn[1][DV:]), (0, 0))
        store(c, 0, pull(part(c, 0, DK) * 0.5, gfq) * 0.5)
        gv = dot3((gn[0][:DV], gn[1][:DV]), attn, (1, 1))
        gfk = dot2r(fq, ga, (1, 1))
        if c < chunks - 1:
            after = halves(rv[c])
            gv = gv + dot2(after, fk, (0, 0))
            gfk = gfk + dot2(after, va[:DV], (1, 0))
            gfk = gfk + dot2(halves(back_norm_at[c]), va[DV:], (0, 0))
        gvs[c] = gv
        gfks[c] = gfk

    collect(rsend, rrecv, rs, rr, -1, rin)
    in_values, in_norms = unpack(rin[...])
    in_pair, in_norm_pair = halves(in_values), halves(in_norms)
    for c in range(chunks):
        fk, va = fks[c], vas[c]
        gv = gvs[c] + dot2(in_pair, fk, (0, 0))
        gfk = gfks[c] + dot2(in_pair, va[:DV], (1, 0)) + dot2(in_norm_pair, va[DV:], (0, 0))
        store(c, DK, gv[: DV // 2])
        store(c, HALF + DK, gv[DV // 2 :])
        store(c, HALF, pull(part(c, DK, DK) * 0.5, gfk) * 0.5)

    pending = shares + ups + qkv
    base = (r // PLANE) * PLANE
    here = pl.ds(base, PLANE)
    there = pl.ds(PLANE - base, PLANE)
    place = r % PLANE
    side = r // PLANE

    def across(i):
        rows = pl.ds(i * ROWS, ROWS)
        for half in range(2):
            pending.append(
                push(
                    o.at[there, half, rows], gj.at[i, 1, 0, core], zs.at[i, half],
                    gr.at[i, 1, 0, core], (g * H + mirror, half),
                )
            )

    def direct(i):
        rows = pl.ds(i * ROWS, ROWS)
        for k in (1, 2):
            for half in range(2):
                pending.append(
                    push(
                        o.at[here, half, rows], gj.at[i, 0, k, core], gs.at[i, 0, k, half],
                        gr.at[i, 0, k, core], (g * H + flip(r, k), half),
                    )
                )
        pending.append(
            push(
                o.at[here, other, rows], gj.at[i, 0, 0, core], gs.at[i, 0, 0, 0],
                gr.at[i, 0, 0, core], (seq, other),
            )
        )

    def landed(ref, sem):
        pltpu.make_async_copy(ref, ref, sem).wait()

    def arrive(i, m, k):
        if m == 0 or k == 0:
            if k < PLANE - 1:
                for b in range(2):
                    landed(gj.at[i, m, k, b], gr.at[i, m, k, b])
                return
        landed(gj.at[i, m, k], gr.at[i, m, k, 0])

    def mirrored(i):
        arrive(i, 1, 0)
        for k in (1, 2):
            pending.append(
                push(
                    gj.at[i, 1, 0], gj.at[i, 1, k], gs.at[i, 1, k, 0], gr.at[i, 1, k, 0], mate(k)
                )
            )

    def turn(i, m):
        return 1 + (i + m) % 2

    def forward(i, m):
        k = turn(i, m)
        arrive(i, m, k)
        pending.append(
            push(
                gj.at[i, m, k], gj.at[i, m, PLANE - 1], hs.at[i, m],
                gr.at[i, m, PLANE - 1, 0], mate(PLANE - 1 - k),
            )
        )

    def multiply(i, m):
        arrive(i, m, PLANE - 1 - turn(i, m))
        arrive(i, m, PLANE - 1)
        if m == 0:
            landed(gj.at[i, 0, 0, other], gr.at[i, 0, 0, other])
        pending.append(
            push(
                gj.at[i, m, :, other, place], rt.at[core, i, m], ts.at[i, m], tr.at[i, m],
                (seq, other),
            )
        )
        rt[core, i, m] = gj[i, m, :, core, place]
        rows = []
        for k in range(PLANE):
            rows.append(
                jnp.concatenate([gj[i, m, k, b, j] for b in range(2) for j in range(PLANE)], 1)
            )
        grads = jnp.concatenate(rows, 0).astype(BF)
        product = dot(grads, xb[...].reshape(2 * PLANE * length, slots * owned), (1, 0))
        for a in range(slots):
            ls[i, m, a % 2, a // 2] = product[:, a * owned : (a + 1) * owned]
        pending.append(
            push(
                ls.at[i, m, 1 - side], lr.at[i, 1 - m], bs.at[i, m], br.at[i, 1 - m], mate(PLANE)
            )
        )

    def combine(i, m):
        landed(lr.at[i, m], br.at[i, m])
        for a in range(ng):
            acc[i, m, a] = ls[i, m, side, a] + lr[i, m, a]
        for d in range(1, ng):
            to = (g + d) % ng
            pending.append(
                push(
                    acc.at[i, m, to], l2.at[i, m, d], cs.at[i, m, d], cr.at[i, m, d],
                    (to * H + r, core),
                )
            )

    swaps = []

    def settled(i):
        for m in range(2):
            total = acc[i, m, g]
            for d in range(1, ng):
                landed(l2.at[i, m, d], cr.at[i, m, d])
                total = total + l2[i, m, d]
            for k in range(PLANE):
                f2[core, i, flip(mirror if m else r, k)] = total[k * ROWS : (k + 1) * ROWS]
        swaps.append(push(f2.at[core, i], f2.at[core, i], ds.at[i], dr.at[i], (seq, other)))

    order = [(0, 0)]
    for i in range(1, PIECES):
        order += [(i, 0), (i - 1, 1)]
    order.append((PIECES - 1, 1))

    def spread(u):
        i, m = order[u]
        if m == 0:
            direct(i)
        else:
            mirrored(i)

    def relayed(u):
        forward(*order[u])

    def product_of(u):
        i, m = order[u]
        multiply(i, m)
        if m == 1:
            combine(i, 1)

    def joined(u):
        i, m = order[u]
        if m == 1:
            combine(i, 0)

    def done(u):
        i, m = order[u]
        if m == 1:
            settled(i)

    units = 2 * PIECES
    stages = list(zip((spread, relayed, product_of, joined, done), LAGS))

    def run(begin, end, only):
        for t in range(begin, end):
            for n, (stage, lag) in enumerate(stages):
                if n in only and 0 <= t - lag < units:
                    stage(t - lag)

    for i in range(PIECES):
        across(i)
        if i < LEAD:
            spread(i)
    for i in range(PIECES):
        gj[i, 0, 0, core] = o[here, core, i * ROWS : (i + 1) * ROWS, :]
    for k in range(1, PLANE):
        shares[k - 1].wait_recv()
        nears.append(swap(k))
    pending += nears
    relayed(0)
    for copy in nears:
        copy.wait_recv()
    for j in range(PLANE):
        xb[core, j * length : (j + 1) * length, :] = xg[base + j].astype(BF)
        xb[other, j * length : (j + 1) * length, :] = xp[base + j].astype(BF)
    every = range(5)
    stop = units + LAGS[2]
    first_turn = max(LEAD, LAGS[1] + 1)
    if LEAD < first_turn:
        run(LEAD, first_turn, (0,))
    run(LAGS[1] + 1, LEAD, every[1:])
    run(first_turn, stop, every)
    for u in range(stop - LAGS[3], units - 1):
        joined(u)
    for i in range(PIECES):
        for m in range(2):
            landed(rt.at[other, i, m], tr.at[i, m])

    def back_rows(h, half):
        low = [((h // bit + r // bit) % 2) * bit for bit in (1, 2)]
        m = (h // PLANE + r // PLANE) % 2
        return jnp.concatenate([rt[half, i, m, low[0] + low[1]] for i in range(PIECES)], 0)

    whole = [[back_rows(h, half) for half in range(2)] for h in range(H)]
    blocks = [jnp.concatenate([whole[h][n][:DK] for h in range(H)], 0) for n in range(2)]
    for h in range(H):
        blocks.append(jnp.concatenate([whole[h][0][DK:], whole[h][1][DK:]], 0))
    for n, block in enumerate(blocks):
        jt[:, n * DV : (n + 1) * DV] = block.T.astype(BF)
    stores = []

    def flow(begin, end, step):
        for at in range(begin, end, step):
            rows = slice(at, at + step)
            total = dot(jt[:, :DV], wq_ref[rows, :], (1, 1))
            total = total + dot(jt[:, DV : 2 * DV], wk_ref[rows, :], (1, 1))
            total = total + dot(jt[:, 2 * DV :], wv_ref[rows, :], (1, 1))
            gi_ref[:, rows] = total.astype(BF)
            copy = pltpu.make_async_copy(
                gi_ref.at[:, rows], gi_hbm.at[:, rows], save.at[at // step]
            )
            copy.start()
            stores.append(copy)

    flow(0, width // 2, width // 4)
    joined(units - 1)
    flow(width // 2, width, width // 4)

    for u in range(stop - LAGS[4], units):
        done(u)
    for copy in swaps:
        copy.wait_recv()
    whole = [
        [jnp.concatenate([f2[n, i, h] for i in range(PIECES)], 0) for n in range(2)]
        for h in range(H)
    ]
    final = [jnp.concatenate([whole[h][n][:DK] for h in range(H)], 0) for n in range(2)]
    for h in range(H):
        final.append(jnp.concatenate([whole[h][0][DK:], whole[h][1][DK:]], 0))
    keep = owned // 2
    for n, block in enumerate(final):
        fs[n] = block.T
        out_ref[n] = fs[n, pl.ds(pl.multiple_of(core * keep, keep), keep), :]
    pending += swaps
    for copy in pending:
        copy.wait_send()
    for copy in stores:
        copy.wait()
    settle(ssend, srecv, ss, sr, 1)
    settle(rsend, rrecv, rs, rr, -1)


def fused(tokens, upstream, weights, ng):
    length, width = tokens.shape
    owned = width // (ng * H)
    slots = 2 * ng
    chunks, span = H // 2, 2 * length
    vm = lambda *shape: pltpu.VMEM(shape, F32)
    half = lambda *shape: pltpu.VMEM(shape, BF)
    state = (FEATS + 16, DV)
    scratch = [half(length, width), half(length, width), half(length, H * DV)]
    scratch += [pltpu.VMEM(w.shape, w.dtype) for w in weights]
    scratch += [
        vm(H, 2 * DK + 2 * DV, length), vm(H, 2 * DK + 2 * DV, length),
        vm(PLANE, length, slots * owned), vm(H, length, slots * owned),
        vm(H, length, slots * owned), half(2, PLANE * length, slots * owned),
        half(chunks, FEATS, span), half(chunks, FEATS, span), half(chunks, DV + AUX, span),
        half(chunks, span, span), half(chunks, span, span),
        half(chunks, DV + AUX, span), half(chunks, DV + AUX, span),
        vm(chunks, DV + AUX, span), vm(chunks, FEATS, DV), vm(chunks, FEATS, DV),
        vm(chunks, DV, span), vm(chunks, FEATS, span),
        vm(*state), vm(ng, *state), vm(*state), vm(*state), vm(ng, *state), vm(*state),
        vm(H, 2, HALF, length), vm(PIECES, 2, PLANE, 2, PLANE, ROWS, length),
        vm(PIECES, 2, 2, ng, PLANE * ROWS, owned), vm(PIECES, 2, ng, PLANE * ROWS, owned),
        vm(PIECES, 2, ng, PLANE * ROWS, owned), vm(PIECES, 2, ng, PLANE * ROWS, owned),
        vm(2, PIECES, 2, PLANE, ROWS, length), half(length, H * DV + 2 * DV),
        vm(2, PIECES, H, ROWS, owned), vm(2 + H, owned, DV),
        sems(5), sems(4),
        sems(H), sems(H), sems(H), sems(H), sems(PLANE), sems(PLANE),
        sems(PLANE), sems(PLANE), sems(ng), sems(ng), sems(ng), sems(ng),
        sems(PIECES, 2), sems(PIECES, 2, PLANE, 2), sems(PIECES, 2, PLANE, 2), sems(PIECES, 2),
        sems(PIECES, 2), sems(PIECES, 2), sems(PIECES, 2), sems(PIECES, 2),
        sems(PIECES, 2, ng), sems(PIECES, 2, ng), sems(PIECES), sems(PIECES),
    ]
    return pl.pallas_call(
        functools.partial(fused_kernel, ng),
        out_shape=[
            jax.ShapeDtypeStruct((length, width), BF),
            jax.ShapeDtypeStruct((2 + H, owned // 2, DV), F32),
        ],
        in_specs=[HBM] * 5,
        out_specs=[HBM, VMEM],
        scratch_shapes=scratch,
        compiler_params=pltpu.CompilerParams(
            collective_id=0, has_side_effects=True, vmem_limit_bytes=60 << 20
        ),
    )(tokens, upstream, *weights)


def finish_kernel(gi_ref, o_ref, in_ref, oq_ref, ok_ref, ov_ref, grad, held, into, out):
    parts = into.shape[0] - 1
    rows = gi_ref.shape[0] // parts
    loads = [pltpu.make_async_copy(o_ref, held, into.at[parts])]
    for n in range(parts):
        at = pl.ds(n * rows, rows)
        loads.append(pltpu.make_async_copy(gi_ref.at[at], grad.at[at], into.at[n]))
    for copy in loads:
        copy.start()
    loads[0].wait()
    stores = [
        pltpu.make_async_copy(held.at[0], oq_ref, out.at[0]),
        pltpu.make_async_copy(held.at[1], ok_ref, out.at[1]),
    ]
    for n in range(H):
        columns = pl.ds(n * DV, DV)
        stores.append(
            pltpu.make_async_copy(held.at[2 + n], ov_ref.at[:, columns], out.at[2 + n])
        )
    for copy in stores:
        copy.start()
    for n in range(parts):
        at = pl.ds(n * rows, rows)
        loads[1 + n].wait()
        copy = pltpu.make_async_copy(grad.at[at], in_ref.at[0, at], out.at[2 + H + n])
        copy.start()
        stores.append(copy)
    for copy in stores:
        copy.wait()


def finish(grad_in, blocks):
    _, rows, lanes = blocks.shape
    parts = 4
    return pl.pallas_call(
        finish_kernel,
        out_shape=[
            jax.ShapeDtypeStruct((1,) + grad_in.shape, BF),
            jax.ShapeDtypeStruct((rows, lanes), F32),
            jax.ShapeDtypeStruct((rows, lanes), F32),
            jax.ShapeDtypeStruct((rows, H * lanes), F32),
        ],
        in_specs=[HBM] * 2,
        out_specs=[HBM] * 4,
        scratch_shapes=[
            pltpu.VMEM(grad_in.shape, BF),
            pltpu.VMEM(blocks.shape, F32),
            sems(1 + parts),
            sems(2 + H + parts),
        ],
    )(grad_in, blocks)


def body(inputs, cotangent, w_query, w_key, w_value):
    ng = lax.axis_size("seq") // H
    weights = (w_query, w_key, w_value)
    return tuple(finish(*fused(inputs[0], cotangent[0], weights, ng)))


def solution(mesh):
    in_specs = (P("batch", "seq", None), P("batch", "seq", None), P(), P(), P())
    out_specs = (
        P("batch", "seq", None),
        P(("seq", "batch"), None),
        P(("seq", "batch"), None),
        P(("seq", "batch"), None),
    )
    return jax.shard_map(body, mesh=mesh, in_specs=in_specs, out_specs=out_specs, check_vma=False)
```
